512 devices in a mesh: dp: 4 (over x), expert: 128 (over z, y, core).
Axes of the slice: x: 4, y: 8, z: 8, core: 2. Of those that a mesh axis runs over, the one named last changes fastest.
Arguments:
- expert_down: bfloat16 [49152, 2048], P('expert'), may hold values from -0.125 to 0.125
- out_grad: bfloat16 [65536, 2048], P(('dp', 'expert')), parts along dimension 0, may hold values from -6 to 6
- routes: int32 [65536, 8], P(('dp', 'expert')), parts along dimension 0, may hold values from 0 to 63, all different within a row; in each aligned block of 128 rows (0 to 127, 128 to 255, ...) at most 24 rows name the same one
- gates: float32 [65536, 8], P(('dp', 'expert')), parts along dimension 0, may hold values from 0.1 to 1
Outputs:
- hidden_grad: bfloat16 [65536, 8, 768], P(('dp', 'expert')), parts along dimension 0
The draws below stay inside these ranges and needn't reach their ends.
There are 4 independent parts, one for each index of `dp`. The reference program is written for one: setup_inputs(seed, part) draws one part's arguments, and reference() takes and returns one part's arrays. A program takes and returns all parts, laid end to end along the dimension named above; an argument that names none is the same for every part. Nothing has to cross between parts.
Inputs may be any that keep to these rules, and one draw needn't show every extreme that they name: `routes`: each token names 8 different experts; among the 128 tokens of one device no expert is named more than 24 times.
All inputs are finite; a program needn't handle non-finite values.
Results may differ from the reference program's by a relative error of at most 0.0049.
Values may be sent and summed in bfloat16 or wider, within the bound.
A program may use at most 64 MiB of HBM per device.

```python
import math
import jax
import jax.numpy as jnp
import numpy as np
from jax import lax

D = 2048
FF = 768
TOK_DEV = 128
EXPERTS = 64
TOP = 8
CAP = 24
TOKENS = 16384
N_EXPERT = 128


def shard_levels(rng, dims, shards, least, largest):
    gain, own = 1.0, jax.random.fold_in(rng, 6)
    for axis_at, shards_of in shards:
        heights = jnp.exp(jax.random.uniform(jax.random.fold_in(own, axis_at), (shards_of,), jnp.float32, least / len(shards), largest / len(shards)))
        gain = gain * jnp.repeat(heights, dims[axis_at] // shards_of).reshape([-1 if axis == axis_at else 1 for axis in range(len(dims))])
    return gain


def assign_block(rng, own, number, rows, number_of, top, most, lean):
    ranking = jax.random.permutation(rng, number_of)
    packed, ordinary = shares(number_of, rows * top, most, lean, True), shares(number_of, rows * top, most, lean, False)
    places = jnp.arange(number_of)

    def named(lengths, rotation):
        used = int((lengths > 0).sum())
        fixed = max(1, used // 4)
        moved = fixed + (places - fixed + rotation * (used - fixed)) % max(1, number_of - fixed)
        return jnp.zeros((number_of,), jnp.int32).at[ranking[jnp.where(places < fixed, places, moved)]].set(jnp.asarray(lengths, jnp.int32))

    lengths = jnp.where(number % 4 == 0, named(packed, number // 4), named(ordinary, number - number // 4 - 1))
    mixed = jax.random.permutation(jax.random.fold_in(own, 3), number_of)
    source_of, sink = mixed[0:number_of // 2 * 2:2], mixed[1:number_of // 2 * 2:2]
    slack = jnp.minimum(lengths[source_of] - 1, most - lengths[sink]) // 2
    slack = jnp.where((source_of == ranking[0]) | (sink == ranking[0]) | (lengths[sink] == 0), 0, jnp.maximum(slack, 0))
    moved = jax.random.randint(jax.random.fold_in(own, 4), (number_of // 2,), 0, 1 << 20) % (slack + 1)
    lengths = lengths.at[source_of].add(-moved).at[sink].add(moved)
    items = jnp.searchsorted(jnp.cumsum(lengths), jnp.arange(rows * top), side="right").astype(jnp.int32)
    listing = items.reshape(top, rows).T
    listing = listing[jax.random.permutation(jax.random.fold_in(own, 1), rows)]
    rotation = jax.random.randint(jax.random.fold_in(own, 2), (rows, 1), 0, top)
    return jnp.take_along_axis(listing, (jnp.arange(top)[None, :] + rotation) % top, axis=1)


def shares(amount, total, bound, slope, full):
    loads = [(1 << 20) // math.isqrt(grade ** slope) + 1 for grade in range(1, amount + 1)]
    largest = bound if full else min(bound, max(-(-total // amount), total * loads[0] // sum(loads)))
    least = 1 if total - largest >= amount - 1 else 0
    given, spare = [largest] + [least] * (amount - 1), total - largest - least * (amount - 1)
    while spare > 0:
        movable = [i for i in range(1, amount) if given[i] < largest] or [i for i in range(1, amount) if given[i] < bound]
        mass, budget = sum([loads[i] for i in movable]), spare
        for i in movable:
            extra = min(bound - given[i], max(1, budget * loads[i] // mass), spare)
            given[i] = given[i] + extra
            spare = spare - extra
    return np.array(given)


def centred(key, shape, width, most, cuts=(), held_as=jnp.bfloat16):
    array = jax.random.normal(key, shape, jnp.float32) * width
    if len(cuts) > 0:
        array = shard_levels(key, shape, cuts, -0.22, 0.18) * array
    return jnp.clip(array, min=-most, max=most).astype(held_as)


def setup_inputs(seed: int = 0, part: int = 0) -> dict:
    splits = jax.random.split(jax.random.key(seed), 5)
    own_keys = jax.random.split(jax.random.fold_in(splits[4], part), 5)
    expert_down = centred(splits[0], (EXPERTS * FF, D), D ** -0.5, 0.125, ((0, 128),))
    out_grad = centred(own_keys[1], (TOKENS, D), 1.0, 6.0, ((0, 128),))
    routes_keys = jax.random.split(jax.random.fold_in(own_keys[2], 1), TOKENS // TOK_DEV)
    routes_turns = jax.random.permutation(jax.random.fold_in(own_keys[2], 3), TOKENS // TOK_DEV)
    routes = jax.vmap(lambda own, number: assign_block(jax.random.fold_in(own_keys[2], 2), own, number, TOK_DEV, EXPERTS, TOP, CAP, 2))(routes_keys, routes_turns).reshape((TOKENS, TOP))
    gates = jnp.clip(0.1 + 0.9 * jax.random.uniform(own_keys[3], (TOKENS, TOP), jnp.float32) ** shard_levels(own_keys[3], (TOKENS, TOP), ((0, 128),), -0.2, 0.2), 0.1, 1.0)
    return dict(expert_down=expert_down, out_grad=out_grad, routes=routes, gates=gates)


def block_slots(expert_ids):
    one_hot = (expert_ids[:, None] == jnp.arange(EXPERTS, dtype=jnp.int32)[None, :]).astype(jnp.int32)
    earlier = jnp.cumsum(one_hot, axis=0) - one_hot
    return jnp.sum(earlier * one_hot, axis=1).astype(jnp.int32)


def reference(expert_down, out_grad, routes, gates):
    per_block = TOK_DEV * TOP
    expert_ids = routes.reshape(N_EXPERT, per_block).astype(jnp.int32)
    slots = jax.vmap(block_slots)(expert_ids)
    block_index = jnp.arange(N_EXPERT, dtype=jnp.int32)[:, None]
    source_token = (jnp.arange(per_block, dtype=jnp.int32) // TOP)[None, :] + block_index * TOK_DEV
    position = (expert_ids * (N_EXPERT * CAP) + block_index * CAP + slots).reshape(-1)
    token_table = jnp.zeros((EXPERTS * N_EXPERT * CAP,), jnp.int32).at[position].set(source_token.reshape(-1))
    token_table = token_table.reshape(EXPERTS, N_EXPERT * CAP)
    weights = expert_down.reshape(EXPERTS, FF, D)

    def per_expert(operands):
        rows_index, weight = operands
        routed_rows = out_grad[rows_index]
        return jnp.dot(routed_rows, weight.T, preferred_element_type=jnp.float32).astype(jnp.bfloat16)

    partial_value = lax.map(per_expert, (token_table, weights))
    picked = partial_value.reshape(EXPERTS * N_EXPERT * CAP, FF)[position]
    result = (gates.reshape(-1)[:, None] * picked.astype(jnp.float32)).astype(jnp.bfloat16)
    return result.reshape(TOKENS, TOP, FF)
```

```python
import functools

import jax
import jax.numpy as jnp
from jax import lax
from jax.experimental import pallas as pl
from jax.experimental.pallas import tpu as pltpu
from jax.sharding import PartitionSpec as P

MESH = pl.DeviceIdType.MESH
RING = 8
X_RING = 4
CAP = 24
PAIR = 2 * CAP
REL = (0, 1, 7, 2, 6, 3, 5, 4)
POS = tuple(REL.index(rel) for rel in range(RING))


def position_of(rel):
    return jnp.where(rel == 0, 0, jnp.where(rel <= 4, 2 * rel - 1, 2 * (8 - rel)))


def rel_of(position):
    half = (position + 1) >> 1
    return jnp.where(position & 1 == 1, half, (8 - half) & 7)


def kernel(
    down_ref,
    grad_ref,
    routes_ref,
    routes_t_ref,
    out_ref,
    tok,
    wts,
    rows_x,
    outgoing,
    returned,
    select,
    routes_all,
    slots_all,
    local_sem,
    tz_send,
    tz_recv,
    tp_send,
    tp_recv,
    own_send,
    own_recv,
    wy_send,
    wy_recv,
    wx_send,
    wx_recv,
    r_send,
    r_recv,
    b_send,
    b_recv,
):
    f32, bf16 = jnp.float32, jnp.bfloat16
    local_tokens, width = grad_ref.shape
    hidden = down_ref.shape[0]
    half_tok = local_tokens // 2
    quarter = hidden // 4
    x = lax.axis_index("dp")
    ex = lax.axis_index("expert")
    core = ex % 2
    other = 1 - core
    y = (ex // 2) % RING
    z = ex // (2 * RING)

    def at_z(rel, c):
        return (x, (((z + rel) % RING) * RING + y) * 2 + c)

    def at_y(rel):
        return (x, (z * RING + (y + rel) % RING) * 2 + core)

    def at_x(rel):
        return ((x + rel) % X_RING, ex)

    partner = (x, ex + 1 - 2 * core)
    pending = []

    def send(src, dst, send_sem, recv_sem, device):
        copy = pltpu.make_async_remote_copy(
            src_ref=src,
            dst_ref=dst,
            send_sem=send_sem,
            recv_sem=recv_sem,
            device_id=device,
            device_id_type=MESH,
        )
        copy.start()
        pending.append(copy)

    def await_copy(ref, sem):
        pltpu.make_async_copy(ref, ref, sem).wait()

    own_rows = pl.ds(pl.multiple_of(core * local_tokens, local_tokens), local_tokens)
    load_tok = pltpu.make_async_copy(grad_ref, tok.at[0, own_rows], local_sem.at[0])
    load_wts = pltpu.make_async_copy(down_ref, wts.at[0], local_sem.at[1])
    load_tok.start()
    load_wts.start()

    barrier = pltpu.get_barrier_semaphore()
    peers = [partner, at_y(1), at_y(-1 + RING), at_x(1), at_x(-1 + X_RING)]
    peers += [at_z(rel, c) for rel in range(1, RING) for c in range(2)]
    for peer in peers:
        pl.semaphore_signal(barrier, inc=1, device_id=peer, device_id_type=MESH)
    pl.semaphore_wait(barrier, len(peers))

    def tok_chunk(rel, half, c=None):
        c = core if c is None else c
        start = pl.multiple_of(c * local_tokens + half * half_tok, half_tok)
        return tok.at[POS[rel % RING], pl.ds(start, half_tok)]

    def z_send(direction, k):
        d = k // 2
        if direction == 0:
            half, src, dst, hop = k % 2, -d, -d - 1, 1
        else:
            half, src, dst, hop = 1 - k % 2, d, d + 1, RING - 1
        send(
            tok_chunk(src, half),
            tok_chunk(dst, half),
            tz_send.at[direction, k],
            tz_recv.at[direction, k],
            at_z(hop, core),
        )

    def z_arrival(direction, k):
        d = k // 2
        return (-d - 1, k % 2) if direction == 0 else (d + 1, 1 - k % 2)

    def z_event(k):
        for direction in range(2):
            chunk = z_arrival(direction, k)
            await_copy(tok_chunk(*chunk), tz_recv.at[direction, k])
            if k <= 4:
                z_send(direction, k + 2)
            send(
                tok_chunk(*chunk),
                tok_chunk(*chunk),
                tp_send.at[direction, k],
                tp_recv.at[direction, k],
                partner,
            )

    def partner_event(k):
        for direction in range(2):
            await_copy(tok_chunk(*z_arrival(direction, k), other), tp_recv.at[direction, k])

    base = 2 * (x % 2)

    def w_chunk(rel, part, quarters):
        start = pl.multiple_of((quarters + part) * quarter, quarter)
        return wts.at[POS[rel % RING], pl.ds(start, quarter)]

    def y_send(direction, k):
        d = k // 2
        if direction == 0:
            part, src, dst, hop = k % 2, -d, -d - 1, 1
        else:
            part, src, dst, hop = 1 - k % 2, d, d + 1, RING - 1
        send(
            w_chunk(src, part, base),
            w_chunk(dst, part, base),
            wy_send.at[direction, k],
            wy_recv.at[direction, k],
            at_y(hop),
        )

    def y_event(k):
        for direction in range(2):
            rel, part = z_arrival(direction, k)
            await_copy(w_chunk(rel, part, base), wy_recv.at[direction, k])
            if k <= 4:
                y_send(direction, k + 2)
            send(
                w_chunk(rel, part, base),
                w_chunk(rel, part, base),
                wx_send.at[part, k],
                wx_recv.at[part, k],
                at_x(X_RING - 1 if part == 0 else 1),
            )

    def x_event(k):
        for direction in range(2):
            rel, part = z_arrival(direction, k)
            await_copy(w_chunk(rel, part, 2 - base), wx_recv.at[part, k])

    def gather(q):
        slots = jnp.concatenate([slots_all[q, 0], slots_all[q, 1]], axis=1)
        number = lax.broadcasted_iota(jnp.int32, (PAIR, 2 * local_tokens), 0).astype(f32)
        pick = jnp.concatenate(
            [jnp.where(slots[p : p + 1, :] == number, 1.0, 0.0) for p in range(RING)], axis=0
        ).astype(bf16)
        cols = 512

        def body(n, carry):
            span = pl.ds(pl.multiple_of(n * cols, cols), cols)
            got = jnp.dot(pick, tok[q, :, span], preferred_element_type=f32)
            rows_x[:, q * PAIR : (q + 1) * PAIR, span] = got.astype(bf16).reshape(RING, PAIR, cols)
            return carry

        lax.fori_loop(0, width // cols, body, 0)

    def multiply(pair, first, last):
        products = []
        for p in (2 * pair, 2 * pair + 1):
            value = lax.dot_general(
                rows_x[p, first * PAIR : last * PAIR, :],
                wts[p],
                (((1,), (1,)), ((), ())),
                preferred_element_type=f32,
            )
            products.append(value.reshape(2 * (last - first), CAP, hidden))
        both = jnp.concatenate(products, axis=1).astype(bf16)
        outgoing[pair, 2 * first : 2 * last] = both

    def send_back(pair, positions):
        for q in positions:
            rel = REL[q]
            if q == 0:
                returned[core, pair, 0] = outgoing[pair, core]
                send(
                    outgoing.at[pair, other],
                    returned.at[core, pair, 0],
                    b_send.at[pair, 0, 0],
                    b_recv.at[pair, 0, 0],
                    partner,
                )
                continue
            for c in range(2):
                send(
                    outgoing.at[pair, 2 * q + c],
                    returned.at[core, pair, POS[(RING - rel) % RING]],
                    b_send.at[pair, q, c],
                    b_recv.at[pair, POS[(RING - rel) % RING], core],
                    at_z(rel, c),
                )

    def assemble(pair):
        await_copy(returned.at[other, pair, 0], b_recv.at[pair, 0, 0])
        for q in range(1, RING):
            for c in range(2):
                await_copy(returned.at[c, pair, q], b_recv.at[pair, q, c])
        rows = local_tokens

        for c in range(2):
            block = returned[c, pair].reshape(RING * PAIR, hidden)

            def body(n, carry):
                span = pl.ds(pl.multiple_of(n * rows, rows), rows)
                got = jnp.dot(
                    select[span, pair * RING * PAIR : (pair + 1) * RING * PAIR],
                    block,
                    preferred_element_type=f32,
                ).astype(bf16)
                columns = slice(c * hidden, (c + 1) * hidden)
                if pair == 0:
                    out_ref[span, columns] = got
                else:
                    out_ref[span, columns] = out_ref[span, columns] + got
                return carry

            lax.fori_loop(0, out_ref.shape[0] // rows, body, 0)

    def home_selection():
        top = routes_ref.shape[1]
        routes = routes_ref[...]
        lane = lax.broadcasted_iota(jnp.int32, (local_tokens, local_tokens), 1)
        sub = lax.broadcasted_iota(jnp.int32, (local_tokens, local_tokens), 0)
        named = jnp.zeros((local_tokens, local_tokens), f32)
        for j in range(top):
            named = jnp.where(routes[:, j : j + 1] == lane, 1.0, named)
        earlier = jnp.where(lane < sub, 1.0, 0.0).astype(bf16)
        counts = jnp.dot(earlier, named.astype(bf16), preferred_element_type=f32).astype(bf16)
        routes_b = routes.astype(f32).astype(bf16)
        p = position_of(((lane & 7) - y + RING) & 7)
        q = position_of(((lane >> 3) - z + 2 * RING) & 7)
        first = ((p >> 1) * (RING * PAIR) + q * PAIR + (p & 1) * CAP).astype(f32)
        lane_f = lane.astype(f32)
        j_lane = lax.broadcasted_iota(jnp.int32, (local_tokens, top), 1)
        j_sub = lax.broadcasted_iota(jnp.int32, (local_tokens, top), 0)
        columns = RING * PAIR
        number = lax.broadcasted_iota(jnp.int32, (local_tokens, columns), 1).astype(f32)

        def body(n, carry):
            token = n * (local_tokens // top) + (sub >> 3)
            repeat = jnp.where(token == lane, 1.0, 0.0).astype(bf16)
            chosen = jnp.dot(repeat, routes_b, preferred_element_type=f32)
            chosen = jnp.sum(jnp.where(j_lane == (j_sub & 7), chosen, 0.0), axis=1, keepdims=True)
            slot = jnp.dot(repeat, counts, preferred_element_type=f32)
            place = jnp.sum(jnp.where(lane_f == chosen, slot + first, 0.0), axis=1, keepdims=True)
            span = pl.ds(pl.multiple_of(n * local_tokens, local_tokens), local_tokens)
            for pair in range(RING // 2):
                hit = jnp.where(place == number + float(pair * columns), 1.0, 0.0)
                select[span, pair * columns : (pair + 1) * columns] = hit.astype(bf16)
            return carry

        lax.fori_loop(0, top, body, 0)

    def source_slots():
        sub = lax.broadcasted_iota(jnp.int32, (RING, local_tokens), 0)
        expert = z * RING + ((y + rel_of(sub)) & 7)
        named = []
        for q in range(RING):
            for s in range(2):
                value = jnp.zeros((RING, local_tokens), f32)
                for j in range(RING):
                    value = jnp.where(routes_all[q, s, j : j + 1, :] == expert, 1.0, value)
                named.append(value)
        named = jnp.concatenate(named, axis=0)
        a = lax.broadcasted_iota(jnp.int32, (local_tokens, local_tokens), 0)
        b = lax.broadcasted_iota(jnp.int32, (local_tokens, local_tokens), 1)
        before = jnp.where(a < b, 1.0, 0.0).astype(bf16)
        counts = jnp.dot(named.astype(bf16), before, preferred_element_type=f32)
        row = lax.broadcasted_iota(jnp.int32, named.shape, 0)
        counts = counts + jnp.where((row >> 3) & 1 == 1, float(CAP), 0.0)
        slots_all[...] = jnp.where(named > 0.5, counts, -1.0).reshape(slots_all.shape)

    load_tok.wait()
    for k in range(2):
        for direction in range(2):
            z_send(direction, k)
    for rel in range(1, RING):
        for c in range(2):
            send(
                routes_t_ref,
                routes_all.at[POS[RING - rel], core],
                r_send.at[POS[rel], c],
                r_recv.at[POS[RING - rel], core],
                at_z(rel, c),
            )
    send(routes_t_ref, routes_all.at[0, core], r_send.at[0, 0], r_recv.at[0, 0], partner)
    load_wts.wait()
    for k in range(2):
        for direction in range(2):
            y_send(direction, k)
    send(tok.at[0, own_rows], tok.at[0, own_rows], own_send, own_recv, partner)
    routes_all[0, core] = routes_t_ref[...]

    home_selection()
    await_copy(routes_all.at[0, other], r_recv.at[0, 0])
    for q in range(1, RING):
        for c in range(2):
            await_copy(routes_all.at[q, c], r_recv.at[q, c])
    source_slots()
    other_rows = pl.ds(pl.multiple_of(other * local_tokens, local_tokens), local_tokens)
    await_copy(tok.at[0, other_rows], own_recv)
    gather(0)

    z_event(0)
    y_event(0)
    z_event(1)
    partner_event(0)
    partner_event(1)
    gather(1)
    gather(2)
    y_event(1)
    z_event(2)
    x_event(0)
    z_event(3)
    partner_event(2)
    partner_event(3)
    gather(3)
    gather(4)
    y_event(2)
    z_event(4)
    x_event(1)
    y_event(3)
    z_event(5)
    partner_event(4)
    partner_event(5)
    gather(5)
    gather(6)
    multiply(0, 0, 7)
    send_back(0, (5, 6, 3, 4, 1, 2, 0))
    x_event(2)
    z_event(6)
    partner_event(6)
    gather(7)
    multiply(0, 7, 8)
    send_back(0, (7,))
    y_event(4)
    x_event(3)
    order = (7, 5, 6, 3, 4, 1, 2, 0)
    multiply(1, 0, 8)
    send_back(1, order)
    y_event(5)
    assemble(0)
    x_event(4)
    y_event(6)
    x_event(5)
    multiply(2, 0, 8)
    send_back(2, order)
    assemble(1)
    x_event(6)
    multiply(3, 0, 8)
    send_back(3, order)
    assemble(2)
    assemble(3)
    for copy in pending:
        copy.wait_send()


def shards(expert_down, out_grad, routes, gates):
    hidden, width = expert_down.shape
    local_tokens, top = routes.shape
    bf16 = jnp.bfloat16
    dma = pltpu.SemaphoreType.DMA
    picked = pl.pallas_call(
        kernel,
        out_shape=jax.ShapeDtypeStruct((local_tokens * top, 2 * hidden), bf16),
        in_specs=[pl.BlockSpec(memory_space=pl.ANY)] * 2
        + [pl.BlockSpec(memory_space=pltpu.VMEM)] * 2,
        out_specs=pl.BlockSpec(memory_space=pltpu.VMEM),
        scratch_shapes=[
            pltpu.VMEM((RING, 2 * local_tokens, width), bf16),
            pltpu.VMEM((RING, hidden, width), bf16),
            pltpu.VMEM((RING, RING * PAIR, width), bf16),
            pltpu.VMEM((RING // 2, 2 * RING, PAIR, hidden), bf16),
            pltpu.VMEM((2, RING // 2, RING, PAIR, hidden), bf16),
            pltpu.VMEM((local_tokens * top, RING * RING * CAP), bf16),
            pltpu.VMEM((RING, 2, top, local_tokens), jnp.int32),
            pltpu.VMEM((RING, 2, RING, local_tokens), jnp.float32),
            dma((2,)),
            dma((2, 7)),
            dma((2, 7)),
            dma((2, 7)),
            dma((2, 7)),
            dma(()),
            dma(()),
            dma((2, 7)),
            dma((2, 7)),
            dma((2, 7)),
            dma((2, 7)),
            dma((RING, 2)),
            dma((RING, 2)),
            dma((RING // 2, RING, 2)),
            dma((RING // 2, RING, 2)),
        ],
        compiler_params=pltpu.CompilerParams(
            collective_id=0, has_side_effects=True, vmem_limit_bytes=60 * 2**20
        ),
    )(expert_down, out_grad, routes, routes.T)
    picked = picked.reshape(local_tokens, top, 2 * hidden)
    return (gates[:, :, None] * picked.astype(jnp.float32)).astype(bf16)


def solution(mesh):
    placed = (
        P("expert", None),
        P(("dp", "expert"), None),
        P(("dp", "expert"), None),
        P(("dp", "expert"), None),
    )
    return jax.shard_map(
        shards,
        mesh=mesh,
        in_specs=placed,
        out_specs=P(("dp", "expert"), None, None),
        check_vma=False,
    )
```

```python
import functools

import jax
import jax.numpy as jnp
from jax import lax
from jax.experimental import pallas as pl
from jax.experimental.pallas import tpu as pltpu
from jax.sharding import PartitionSpec as P

MESH = pl.DeviceIdType.MESH
RING = 8
X_RING = 4
CAP = 24
PAIR = 2 * CAP
REL = (0, 1, 7, 2, 6, 3, 5, 4)
POS = tuple(REL.index(rel) for rel in range(RING))
GROUPS = ((0, 1), (2, 3), (4,), (5, 6), (7,))
STARTS = tuple(sum(len(g) for g in GROUPS[:n]) * RING * CAP for n in range(len(GROUPS)))


def position_of(rel):
    return jnp.where(rel == 0, 0, jnp.where(rel <= 4, 2 * rel - 1, 2 * (8 - rel)))


def rel_of(position):
    half = (position + 1) >> 1
    return jnp.where(position & 1 == 1, half, (8 - half) & 7)


def kernel(
    down_ref,
    grad_ref,
    routes_t_ref,
    gates_t_ref,
    out_ref,
    returned_4,
    select_4,
    scale,
    tok,
    wts,
    rows_x,
    outgoing_0,
    outgoing_1,
    outgoing_2,
    outgoing_3,
    outgoing_4,
    returned_0,
    returned_1,
    returned_2,
    returned_3,
    select,
    routes_all,
    slots_all,
    local_sem,
    tz_send,
    tz_recv,
    tp_send,
    tp_recv,
    own_send,
    own_recv,
    wy_send,
    wy_recv,
    wx_send,
    wx_recv,
    r_send,
    r_recv,
    b_send,
    b_recv,
):
    f32, bf16 = jnp.float32, jnp.bfloat16
    outgoing = (outgoing_0, outgoing_1, outgoing_2, outgoing_3, outgoing_4)
    returned = (returned_0, returned_1, returned_2, returned_3, returned_4)
    local_tokens, width = grad_ref.shape
    hidden = down_ref.shape[0]
    half_tok = local_tokens // 2
    quarter = hidden // 4
    x = lax.axis_index("dp")
    ex = lax.axis_index("expert")
    core = ex % 2
    other = 1 - core
    y = (ex // 2) % RING
    z = ex // (2 * RING)

    def at_z(rel, c):
        return (x, (((z + rel) % RING) * RING + y) * 2 + c)

    def at_y(rel):
        return (x, (z * RING + (y + rel) % RING) * 2 + core)

    def at_x(rel):
        return ((x + rel) % X_RING, ex)

    partner = (x, ex + 1 - 2 * core)
    pending = []

    def send(src, dst, send_sem, recv_sem, device):
        copy = pltpu.make_async_remote_copy(
            src_ref=src,
            dst_ref=dst,
            send_sem=send_sem,
            recv_sem=recv_sem,
            device_id=device,
            device_id_type=MESH,
        )
        copy.start()
        pending.append(copy)

    def await_copy(ref, sem):
        pltpu.make_async_copy(ref, ref, sem).wait()

    own_rows = pl.ds(pl.multiple_of(core * local_tokens, local_tokens), local_tokens)
    load_tok = pltpu.make_async_copy(grad_ref, tok.at[0, own_rows], local_sem.at[0])
    load_wts = pltpu.make_async_copy(down_ref, wts.at[0], local_sem.at[1])
    load_tok.start()
    load_wts.start()

    barrier = pltpu.get_barrier_semaphore()
    peers = [partner, at_y(1), at_y(-1 + RING), at_x(1), at_x(-1 + X_RING)]
    peers += [at_z(rel, c) for rel in range(1, RING) for c in range(2)]
    for peer in peers:
        pl.semaphore_signal(barrier, inc=1, device_id=peer, device_id_type=MESH)
    pl.semaphore_wait(barrier, len(peers))

    def tok_chunk(rel, half, c=None):
        c = core if c is None else c
        start = pl.multiple_of(c * local_tokens + half * half_tok, half_tok)
        return tok.at[POS[rel % RING], pl.ds(start, half_tok)]

    def z_send(direction, k):
        d = k // 2
        if direction == 0:
            half, src, dst, hop = k % 2, -d, -d - 1, 1
        else:
            half, src, dst, hop = 1 - k % 2, d, d + 1, RING - 1
        send(
            tok_chunk(src, half),
            tok_chunk(dst, half),
            tz_send.at[direction, k],
            tz_recv.at[direction, k],
            at_z(hop, core),
        )

    def z_arrival(direction, k):
        d = k // 2
        return (-d - 1, k % 2) if direction == 0 else (d + 1, 1 - k % 2)

    def z_event(k):
        for direction in range(2):
            chunk = z_arrival(direction, k)
            await_copy(tok_chunk(*chunk), tz_recv.at[direction, k])
            if k <= 4:
                z_send(direction, k + 2)
            send(
                tok_chunk(*chunk),
                tok_chunk(*chunk),
                tp_send.at[direction, k],
                tp_recv.at[direction, k],
                partner,
            )

    def partner_event(k):
        for direction in range(2):
            await_copy(tok_chunk(*z_arrival(direction, k), other), tp_recv.at[direction, k])

    base = 2 * (x % 2)

    def w_chunk(rel, part, quarters):
        start = pl.multiple_of((quarters + part) * quarter, quarter)
        return wts.at[POS[rel % RING], pl.ds(start, quarter)]

    def y_send(direction, k):
        d = k // 2
        if direction == 0:
            part, src, dst, hop = k % 2, -d, -d - 1, 1
        else:
            part, src, dst, hop = 1 - k % 2, d, d + 1, RING - 1
        send(
            w_chunk(src, part, base),
            w_chunk(dst, part, base),
            wy_send.at[direction, k],
            wy_recv.at[direction, k],
            at_y(hop),
        )

    def y_event(k):
        for direction in range(2):
            rel, part = z_arrival(direction, k)
            await_copy(w_chunk(rel, part, base), wy_recv.at[direction, k])
            if k <= 4:
                y_send(direction, k + 2)
            send(
                w_chunk(rel, part, base),
                w_chunk(rel, part, base),
                wx_send.at[part, k],
                wx_recv.at[part, k],
                at_x(X_RING - 1 if part == 0 else 1),
            )

    def x_event(k):
        for direction in range(2):
            rel, part = z_arrival(direction, k)
            await_copy(w_chunk(rel, part, 2 - base), wx_recv.at[part, k])

    def gather(q):
        slots = jnp.concatenate([slots_all[q, 0], slots_all[q, 1]], axis=1)
        number = lax.broadcasted_iota(jnp.int32, (PAIR, 2 * local_tokens), 0).astype(f32)
        pick = jnp.concatenate(
            [jnp.where(slots[p : p + 1, :] == number, 1.0, 0.0) for p in range(RING)], axis=0
        ).astype(bf16)
        cols = 512

        def body(n, carry):
            span = pl.ds(pl.multiple_of(n * cols, cols), cols)
            got = jnp.dot(pick, tok[q, :, span], preferred_element_type=f32)
            rows_x[:, q * PAIR : (q + 1) * PAIR, span] = got.astype(bf16).reshape(RING, PAIR, cols)
            return carry

        lax.fori_loop(0, width // cols, body, 0)

    def multiply(group, first, last):
        products = []
        for p in GROUPS[group]:
            value = lax.dot_general(
                rows_x[p, first * PAIR : last * PAIR, :],
                wts[p],
                (((1,), (1,)), ((), ())),
                preferred_element_type=f32,
            )
            products.append(value.reshape(2 * (last - first), CAP, hidden))
        both = jnp.concatenate(products, axis=1) if len(products) > 1 else products[0]
        outgoing[group][2 * first : 2 * last] = both.astype(bf16)

    def send_back(group, positions):
        for q in positions:
            rel = REL[q]
            if q == 0:
                returned[group][core, 0] = outgoing[group][core]
                send(
                    outgoing[group].at[other],
                    returned[group].at[core, 0],
                    b_send.at[group, 0, 0],
                    b_recv.at[group, 0, 0],
                    partner,
                )
                continue
            for c in range(2):
                send(
                    outgoing[group].at[2 * q + c],
                    returned[group].at[core, POS[(RING - rel) % RING]],
                    b_send.at[group, q, c],
                    b_recv.at[group, POS[(RING - rel) % RING], core],
                    at_z(rel, c),
                )

    def await_returned(group):
        await_copy(returned[group].at[other, 0], b_recv.at[group, 0, 0])
        for q in range(1, RING):
            for c in range(2):
                await_copy(returned[group].at[c, q], b_recv.at[group, q, c])

    def assemble(group):
        await_returned(group)
        rows = 4 * local_tokens
        depth = len(GROUPS[group]) * RING * CAP

        for c in range(2):

            def body(n, carry):
                span = pl.ds(pl.multiple_of(n * rows, rows), rows)
                got = jnp.dot(
                    select[span, STARTS[group] : STARTS[group] + depth],
                    returned[group][c].reshape(depth, hidden),
                    preferred_element_type=f32,
                )
                factor = scale[span, :]
                for col in range(0, hidden, 128):
                    columns = slice(c * hidden + col, c * hidden + col + 128)
                    term = (factor * got[:, col : col + 128]).astype(bf16)
                    if group == 0:
                        out_ref[span, columns] = term
                    else:
                        out_ref[span, columns] = out_ref[span, columns] + term
                return carry

            lax.fori_loop(0, out_ref.shape[0] // rows, body, 0)

    def home_selection():
        top = routes_t_ref.shape[0]
        routes = routes_t_ref[...]
        lane = lax.broadcasted_iota(jnp.int32, (local_tokens, local_tokens), 1)
        sub = lax.broadcasted_iota(jnp.int32, (local_tokens, local_tokens), 0)
        expert_by_token = jnp.zeros((local_tokens, local_tokens), f32)
        for j in range(top):
            expert_by_token = jnp.where(routes[j : j + 1, :] == sub, 1.0, expert_by_token)
        earlier = jnp.where(lane < sub, 1.0, 0.0).astype(bf16)
        counts = lax.dot_general(
            earlier,
            expert_by_token.astype(bf16),
            (((1,), (1,)), ((), ())),
            preferred_element_type=f32,
        ).astype(bf16)
        p = position_of(((lane & 7) - y + RING) & 7)
        q = position_of(((lane >> 3) - z + 2 * RING) & 7)
        first = jnp.zeros(lane.shape, jnp.int32)
        for start, group in zip(STARTS, GROUPS):
            for n, member in enumerate(group):
                row = start + q * (len(group) * CAP) + n * CAP
                first = jnp.where(p == member, row, first)
        first = first.astype(f32)
        lane_f = lane.astype(f32)
        columns = RING * PAIR
        number = lax.broadcasted_iota(jnp.int32, (local_tokens, columns), 1).astype(f32)
        per_step = local_tokens // top
        routes_rows = jnp.concatenate([routes.astype(f32)] * per_step, axis=0)
        gates_rows = jnp.concatenate([gates_t_ref[...]] * per_step, axis=0)

        def body(n, carry):
            here = n * per_step + (sub >> 3) == lane
            repeat = jnp.where(here, 1.0, 0.0).astype(bf16)
            chosen = jnp.sum(jnp.where(here, routes_rows, 0.0), axis=1, keepdims=True)
            gate = jnp.sum(jnp.where(here, gates_rows, 0.0), axis=1, keepdims=True)
            slot = jnp.dot(repeat, counts, preferred_element_type=f32)
            place = jnp.sum(jnp.where(lane_f == chosen, slot + first, 0.0), axis=1, keepdims=True)
            span = pl.ds(pl.multiple_of(n * local_tokens, local_tokens), local_tokens)
            scale[span, :] = jnp.broadcast_to(gate, (local_tokens, scale.shape[1]))
            for start in range(0, STARTS[-1], columns):
                size = min(columns, STARTS[-1] - start)
                hit = jnp.where(place == number[:, :size] + float(start), 1.0, 0.0)
                select[span, start : start + size] = hit.astype(bf16)
            last = jnp.where(place == number[:, : select_4.shape[1]] + float(STARTS[-1]), 1.0, 0.0)
            select_4[span, :] = last.astype(bf16)
            return carry

        lax.fori_loop(0, top, body, 0)

    def source_slots():
        sub = lax.broadcasted_iota(jnp.int32, (RING, local_tokens), 0)
        expert = z * RING + ((y + rel_of(sub)) & 7)
        named = []
        for q in range(RING):
            for s in range(2):
                value = jnp.zeros((RING, local_tokens), f32)
                for j in range(RING):
                    value = jnp.where(routes_all[q, s, j : j + 1, :] == expert, 1.0, value)
                named.append(value)
        named = jnp.concatenate(named, axis=0)
        a = lax.broadcasted_iota(jnp.int32, (local_tokens, local_tokens), 0)
        b = lax.broadcasted_iota(jnp.int32, (local_tokens, local_tokens), 1)
        before = jnp.where(a < b, 1.0, 0.0).astype(bf16)
        counts = jnp.dot(named.astype(bf16), before, preferred_element_type=f32)
        row = lax.broadcasted_iota(jnp.int32, named.shape, 0)
        counts = counts + jnp.where((row >> 3) & 1 == 1, float(CAP), 0.0)
        slots_all[...] = jnp.where(named > 0.5, counts, -1.0).reshape(slots_all.shape)

    for rel in (4, 3, 5, 2, 6, 1, 7):
        for c in range(2):
            send(
                routes_t_ref,
                routes_all.at[POS[RING - rel], core],
                r_send.at[POS[rel], c],
                r_recv.at[POS[RING - rel], core],
                at_z(rel, c),
            )
    send(routes_t_ref, routes_all.at[0, core], r_send.at[0, 0], r_recv.at[0, 0], partner)
    load_tok.wait()
    for k in range(2):
        for direction in range(2):
            z_send(direction, k)
    load_wts.wait()
    for k in range(2):
        for direction in range(2):
            y_send(direction, k)
    send(tok.at[0, own_rows], tok.at[0, own_rows], own_send, own_recv, partner)
    routes_all[0, core] = routes_t_ref[...]

    home_selection()
    await_copy(routes_all.at[0, other], r_recv.at[0, 0])
    for q in range(1, RING):
        for c in range(2):
            await_copy(routes_all.at[q, c], r_recv.at[q, c])
    source_slots()
    other_rows = pl.ds(pl.multiple_of(other * local_tokens, local_tokens), local_tokens)
    await_copy(tok.at[0, other_rows], own_recv)
    z_event(0)
    gather(0)
    y_event(0)
    z_event(1)
    partner_event(0)
    partner_event(1)
    gather(1)
    gather(2)
    z_event(2)
    y_event(1)
    z_event(3)
    partner_event(2)
    partner_event(3)
    gather(3)
    y_event(2)
    gather(4)
    z_event(4)
    z_event(5)
    y_event(3)
    partner_event(4)
    partner_event(5)
    gather(5)
    gather(6)
    x_event(0)
    x_event(1)
    multiply(0, 0, 7)
    send_back(0, (5, 6, 3, 4, 1, 2, 0))
    z_event(6)
    partner_event(6)
    gather(7)
    multiply(0, 7, 8)
    send_back(0, (7,))
    y_event(4)
    order = (7, 5, 6, 3, 4, 1, 2, 0)
    x_event(2)
    x_event(3)
    multiply(1, 0, 8)
    send_back(1, order)
    multiply(2, 0, 8)
    send_back(2, order)
    y_event(5)
    assemble(0)
    y_event(6)
    x_event(4)
    x_event(5)
    multiply(3, 0, 8)
    send_back(3, order)
    assemble(1)
    x_event(6)
    multiply(4, 0, 8)
    send_back(4, order)
    assemble(2)
    assemble(3)
    await_returned(4)
    for copy in pending:
        copy.wait_send()


def finish_kernel(out_ref, returned_4, select_4, scale, final_ref, buffer, sems):
    f32, bf16 = jnp.float32, jnp.bfloat16
    hidden = returned_4.shape[-1]
    rows = buffer.shape[1]
    steps = buffer.shape[0]
    blocks = [returned_4[c].reshape(RING * CAP, hidden) for c in range(2)]
    copies = []
    for n in range(steps):
        span = slice(n * rows, (n + 1) * rows)
        factor = scale[span, :]
        for c in range(2):
            got = jnp.dot(select_4[span, :], blocks[c], preferred_element_type=f32)
            for col in range(0, hidden, 128):
                columns = slice(c * hidden + col, c * hidden + col + 128)
                term = (factor * got[:, col : col + 128]).astype(bf16)
                buffer[n, :, columns] = out_ref[span, columns] + term
        copies.append(pltpu.make_async_copy(buffer.at[n], final_ref.at[span], sems.at[n]))
        if n > 0:
            copies[n - 1].start()
    copies[-1].start()
    for copy in copies:
        copy.wait()


def shards(expert_down, out_grad, routes, gates):
    hidden, width = expert_down.shape
    local_tokens, top = routes.shape
    choices = local_tokens * top
    bf16 = jnp.bfloat16
    dma = pltpu.SemaphoreType.DMA
    vmem = pl.BlockSpec(memory_space=pltpu.VMEM)
    hbm = pl.BlockSpec(memory_space=pl.ANY)
    parts = pl.pallas_call(
        kernel,
        out_shape=(
            pltpu.VMEM((choices, 2 * hidden), bf16),
            pltpu.VMEM((2, RING, CAP, hidden), bf16),
            pltpu.VMEM((choices, RING * CAP), bf16),
            pltpu.VMEM((choices, 128), jnp.float32),
        ),
        in_specs=[hbm, hbm, vmem, vmem],
        out_specs=[vmem] * 4,
        scratch_shapes=[
            pltpu.VMEM((RING, 2 * local_tokens, width), bf16),
            pltpu.VMEM((RING, hidden, width), bf16),
            pltpu.VMEM((RING, RING * PAIR, width), bf16),
            *[pltpu.VMEM((2 * RING, len(g) * CAP, hidden), bf16) for g in GROUPS],
            *[pltpu.VMEM((2, RING, len(g) * CAP, hidden), bf16) for g in GROUPS[:-1]],
            pltpu.VMEM((choices, STARTS[-1]), bf16),
            pltpu.VMEM((RING, 2, top, local_tokens), jnp.int32),
            pltpu.VMEM((RING, 2, RING, local_tokens), jnp.float32),
            dma((2,)),
            dma((2, 7)),
            dma((2, 7)),
            dma((2, 7)),
            dma((2, 7)),
            dma(()),
            dma(()),
            dma((2, 7)),
            dma((2, 7)),
            dma((2, 7)),
            dma((2, 7)),
            dma((RING, 2)),
            dma((RING, 2)),
            dma((len(GROUPS), RING, 2)),
            dma((len(GROUPS), RING, 2)),
        ],
        compiler_params=pltpu.CompilerParams(
            collective_id=0, has_side_effects=True, vmem_limit_bytes=52 * 2**20
        ),
    )(expert_down, out_grad, routes.T, gates.T)
    steps = 8
    final = pl.pallas_call(
        finish_kernel,
        out_shape=jax.ShapeDtypeStruct((choices, 2 * hidden), bf16),
        in_specs=[vmem] * 4,
        out_specs=hbm,
        scratch_shapes=[
            pltpu.VMEM((steps, choices // steps, 2 * hidden), bf16),
            dma((steps,)),
        ],
        compiler_params=pltpu.CompilerParams(vmem_limit_bytes=16 * 2**20),
    )(*parts)
    return final.reshape(local_tokens, top, 2 * hidden)


def solution(mesh):
    placed = (
        P("expert", None),
        P(("dp", "expert"), None),
        P(("dp", "expert"), None),
        P(("dp", "expert"), None),
    )
    return jax.shard_map(
        shards,
        mesh=mesh,
        in_specs=placed,
        out_specs=P(("dp", "expert"), None, None),
        check_vma=False,
    )
```

```python
import functools

import jax
import jax.numpy as jnp
from jax import lax
from jax.experimental import pallas as pl
from jax.experimental.pallas import tpu as pltpu
from jax.sharding import PartitionSpec as P

MESH = pl.DeviceIdType.MESH
RING = 8
X_RING = 4
CAP = 24
PAIR = 2 * CAP
REL = (0, 1, 7, 2, 6, 3, 5, 4)
POS = tuple(REL.index(rel) for rel in range(RING))
GROUPS = ((0, 1), (2, 3), (4,), (5, 6), (7,))
STARTS = tuple(sum(len(g) for g in GROUPS[:n]) * RING * CAP for n in range(len(GROUPS)))


def position_of(rel):
    return jnp.where(rel == 0, 0, jnp.where(rel <= 4, 2 * rel - 1, 2 * (8 - rel)))


def rel_of(position):
    half = (position + 1) >> 1
    return jnp.where(position & 1 == 1, half, (8 - half) & 7)


def kernel(
    down_ref,
    grad_ref,
    routes_t_ref,
    gates_t_ref,
    out_ref,
    returned_4,
    select_4,
    scale,
    tok,
    wts,
    rows_x,
    outgoing_0,
    outgoing_1,
    outgoing_2,
    outgoing_3,
    outgoing_4,
    returned_0,
    returned_1,
    returned_2,
    returned_3,
    select,
    routes_all,
    slots_all,
    local_sem,
    tz_send,
    tz_recv,
    tp_send,
    tp_recv,
    own_recv,
    wy_send,
    wy_recv,
    wx_send,
    wx_recv,
    r_send,
    r_recv,
    rp_send,
    rp_recv,
    b_send,
    b_recv,
    bp_send,
    bp_recv,
):
    f32, bf16 = jnp.float32, jnp.bfloat16
    outgoing = (outgoing_0, outgoing_1, outgoing_2, outgoing_3, outgoing_4)
    returned = (returned_0, returned_1, returned_2, returned_3, returned_4)
    local_tokens, width = grad_ref.shape
    hidden = down_ref.shape[0]
    half_tok = local_tokens // 2
    quarter = hidden // 4
    x = lax.axis_index("dp")
    ex = lax.axis_index("expert")
    core = ex % 2
    other = 1 - core
    y = (ex // 2) % RING
    z = ex // (2 * RING)

    def at_z(rel, c):
        return (x, (((z + rel) % RING) * RING + y) * 2 + c)

    def at_y(rel):
        return (x, (z * RING + (y + rel) % RING) * 2 + core)

    def at_x(rel):
        return ((x + rel) % X_RING, ex)

    partner = (x, ex + 1 - 2 * core)

    def send(src, dst, send_sem, recv_sem, device):
        copy = pltpu.make_async_remote_copy(
            src_ref=src,
            dst_ref=dst,
            send_sem=send_sem,
            recv_sem=recv_sem,
            device_id=device,
            device_id_type=MESH,
        )
        copy.start()

    def await_copy(ref, sem):
        pltpu.make_async_copy(ref, ref, sem).wait()

    own_rows = pl.ds(pl.multiple_of(core * local_tokens, local_tokens), local_tokens)
    load_tok = pltpu.make_async_copy(grad_ref, tok.at[0, own_rows], local_sem.at[0])
    load_wts = pltpu.make_async_copy(down_ref, wts.at[0], local_sem.at[1])
    load_tok.start()
    load_wts.start()

    barrier = pltpu.get_barrier_semaphore()
    peers = [partner, at_y(1), at_y(-1 + RING), at_x(1), at_x(-1 + X_RING)]
    peers += [at_z(rel, c) for rel in range(1, RING) for c in range(2)]
    for peer in peers:
        pl.semaphore_signal(barrier, inc=1, device_id=peer, device_id_type=MESH)
    pl.semaphore_wait(barrier, len(peers))

    def tok_chunk(rel, half, c=None):
        c = core if c is None else c
        start = pl.multiple_of(c * local_tokens + half * half_tok, half_tok)
        return tok.at[POS[rel % RING], pl.ds(start, half_tok)]

    def z_send(direction, k):
        d = k // 2
        if direction == 0:
            half, src, dst, hop = k % 2, -d, -d - 1, 1
        else:
            half, src, dst, hop = 1 - k % 2, d, d + 1, RING - 1
        send(
            tok_chunk(src, half),
            tok_chunk(dst, half),
            tz_send,
            tz_recv.at[direction, k],
            at_z(hop, core),
        )

    def z_arrival(direction, k):
        d = k // 2
        return (-d - 1, k % 2) if direction == 0 else (d + 1, 1 - k % 2)

    def z_event(k):
        for direction in range(2):
            chunk = z_arrival(direction, k)
            await_copy(tok_chunk(*chunk), tz_recv.at[direction, k])
            if k <= 4:
                z_send(direction, k + 2)
            send(
                tok_chunk(*chunk),
                tok_chunk(*chunk),
                tp_send,
                tp_recv.at[direction, k],
                partner,
            )

    def partner_event(k):
        for direction in range(2):
            await_copy(tok_chunk(*z_arrival(direction, k), other), tp_recv.at[direction, k])

    base = 2 * (x % 2)

    def w_chunk(rel, part, quarters):
        start = pl.multiple_of((quarters + part) * quarter, quarter)
        return wts.at[POS[rel % RING], pl.ds(start, quarter)]

    def y_send(direction, k):
        d = k // 2
        if direction == 0:
            part, src, dst, hop = k % 2, -d, -d - 1, 1
        else:
            part, src, dst, hop = 1 - k % 2, d, d + 1, RING - 1
        send(
            w_chunk(src, part, base),
            w_chunk(dst, part, base),
            wy_send,
            wy_recv.at[direction, k],
            at_y(hop),
        )

    def y_event(k):
        for direction in range(2):
            rel, part = z_arrival(direction, k)
            await_copy(w_chunk(rel, part, base), wy_recv.at[direction, k])
            if k <= 4:
                y_send(direction, k + 2)
            send(
                w_chunk(rel, part, base),
                w_chunk(rel, part, base),
                wx_send,
                wx_recv.at[part, k],
                at_x(X_RING - 1 if part == 0 else 1),
            )

    def x_event(k):
        for direction in range(2):
            rel, part = z_arrival(direction, k)
            await_copy(w_chunk(rel, part, 2 - base), wx_recv.at[part, k])

    def gather(q):
        slots = jnp.concatenate([slots_all[q, 0], slots_all[q, 1]], axis=1)
        number = lax.broadcasted_iota(jnp.int32, (PAIR, 2 * local_tokens), 0).astype(f32)
        pick = jnp.concatenate(
            [jnp.where(slots[p : p + 1, :] == number, 1.0, 0.0) for p in range(RING)], axis=0
        ).astype(bf16)
        cols = 512

        def body(n, carry):
            span = pl.ds(pl.multiple_of(n * cols, cols), cols)
            got = jnp.dot(pick, tok[q, :, span], preferred_element_type=f32)
            rows_x[:, q * PAIR : (q + 1) * PAIR, span] = got.astype(bf16).reshape(RING, PAIR, cols)
            return carry

        lax.fori_loop(0, width // cols, body, 0)

    def multiply(group, first, last):
        products = []
        for p in GROUPS[group]:
            value = lax.dot_general(
                rows_x[p, first * PAIR : last * PAIR, :],
                wts[p],
                (((1,), (1,)), ((), ())),
                preferred_element_type=f32,
            )
            products.append(value.reshape(2 * (last - first), CAP, hidden))
        both = jnp.concatenate(products, axis=1) if len(products) > 1 else products[0]
        outgoing[group][2 * first : 2 * last] = both.astype(bf16)

    def send_back(group, positions):
        for q in positions:
            rel = REL[q]
            if q == 0:
                returned[group][core, 0] = outgoing[group][core]
                send(
                    outgoing[group].at[other],
                    returned[group].at[core, 0],
                    bp_send.at[group],
                    bp_recv.at[group],
                    partner,
                )
                continue
            for c in range(2):
                send(
                    outgoing[group].at[2 * q + c],
                    returned[group].at[core, POS[(RING - rel) % RING]],
                    b_send.at[group],
                    b_recv.at[group],
                    at_z(rel, c),
                )

    def await_returned(group):
        await_copy(returned[group].at[other, 0], bp_recv.at[group])
        await_copy(returned[group].at[:, 1:RING], b_recv.at[group])

    def assemble(group):
        await_returned(group)
        rows = 4 * local_tokens
        depth = len(GROUPS[group]) * RING * CAP

        for c in range(2):

            def body(n, carry):
                span = pl.ds(pl.multiple_of(n * rows, rows), rows)
                got = jnp.dot(
                    select[span, STARTS[group] : STARTS[group] + depth],
                    returned[group][c].reshape(depth, hidden),
                    preferred_element_type=f32,
                )
                factor = scale[span, :]
                for col in range(0, hidden, 128):
                    columns = slice(c * hidden + col, c * hidden + col + 128)
                    term = (factor * got[:, col : col + 128]).astype(bf16)
                    if group == 0:
                        out_ref[span, columns] = term
                    else:
                        out_ref[span, columns] = out_ref[span, columns] + term
                return carry

            lax.fori_loop(0, out_ref.shape[0] // rows, body, 0)

    def home_selection():
        top = routes_t_ref.shape[0]
        routes = routes_t_ref[...]
        lane = lax.broadcasted_iota(jnp.int32, (local_tokens, local_tokens), 1)
        sub = lax.broadcasted_iota(jnp.int32, (local_tokens, local_tokens), 0)
        expert_by_token = jnp.zeros((local_tokens, local_tokens), f32)
        for j in range(top):
            expert_by_token = jnp.where(routes[j : j + 1, :] == sub, 1.0, expert_by_token)
        earlier = jnp.where(lane < sub, 1.0, 0.0).astype(bf16)
        counts = lax.dot_general(
            earlier,
            expert_by_token.astype(bf16),
            (((1,), (1,)), ((), ())),
            preferred_element_type=f32,
        ).astype(bf16)
        p = position_of(((lane & 7) - y + RING) & 7)
        q = position_of(((lane >> 3) - z + 2 * RING) & 7)
        first = jnp.zeros(lane.shape, jnp.int32)
        for start, group in zip(STARTS, GROUPS):
            for n, member in enumerate(group):
                row = start + q * (len(group) * CAP) + n * CAP
                first = jnp.where(p == member, row, first)
        first = first.astype(f32)
        lane_f = lane.astype(f32)
        columns = RING * PAIR
        number = lax.broadcasted_iota(jnp.int32, (local_tokens, columns), 1).astype(f32)
        per_step = local_tokens // top
        routes_rows = jnp.concatenate([routes.astype(f32)] * per_step, axis=0)
        gates_rows = jnp.concatenate([gates_t_ref[...]] * per_step, axis=0)

        def body(n, carry):
            here = n * per_step + (sub >> 3) == lane
            repeat = jnp.where(here, 1.0, 0.0).astype(bf16)
            chosen = jnp.sum(jnp.where(here, routes_rows, 0.0), axis=1, keepdims=True)
            gate = jnp.sum(jnp.where(here, gates_rows, 0.0), axis=1, keepdims=True)
            slot = jnp.dot(repeat, counts, preferred_element_type=f32)
            place = jnp.sum(jnp.where(lane_f == chosen, slot + first, 0.0), axis=1, keepdims=True)
            span = pl.ds(pl.multiple_of(n * local_tokens, local_tokens), local_tokens)
            scale[span, :] = jnp.broadcast_to(gate, (local_tokens, scale.shape[1]))
            for start in range(0, STARTS[-1], columns):
                size = min(columns, STARTS[-1] - start)
                hit = jnp.where(place == number[:, :size] + float(start), 1.0, 0.0)
                select[span, start : start + size] = hit.astype(bf16)
            last = jnp.where(place == number[:, : select_4.shape[1]] + float(STARTS[-1]), 1.0, 0.0)
            select_4[span, :] = last.astype(bf16)
            return carry

        lax.fori_loop(0, top, body, 0)

    def source_slots():
        sub = lax.broadcasted_iota(jnp.int32, (RING, local_tokens), 0)
        expert = z * RING + ((y + rel_of(sub)) & 7)
        named = []
        for q in range(RING):
            for s in range(2):
                value = jnp.zeros((RING, local_tokens), f32)
                for j in range(RING):
                    value = jnp.where(routes_all[q, s, j : j + 1, :] == expert, 1.0, value)
                named.append(value)
        named = jnp.concatenate(named, axis=0)
        a = lax.broadcasted_iota(jnp.int32, (local_tokens, local_tokens), 0)
        b = lax.broadcasted_iota(jnp.int32, (local_tokens, local_tokens), 1)
        before = jnp.where(a < b, 1.0, 0.0).astype(bf16)
        counts = jnp.dot(named.astype(bf16), before, preferred_element_type=f32)
        row = lax.broadcasted_iota(jnp.int32, named.shape, 0)
        counts = counts + jnp.where((row >> 3) & 1 == 1, float(CAP), 0.0)
        slots_all[...] = jnp.where(named > 0.5, counts, -1.0).reshape(slots_all.shape)

    for rel in (4, 3, 5, 2, 6, 1, 7):
        for c in range(2):
            send(
                routes_t_ref,
                routes_all.at[POS[RING - rel], core],
                r_send,
                r_recv,
                at_z(rel, c),
            )
    send(routes_t_ref, routes_all.at[0, core], rp_send, rp_recv, partner)
    load_tok.wait()
    for k in range(2):
        for direction in range(2):
            z_send(direction, k)
    load_wts.wait()
    for k in range(2):
        for direction in range(2):
            y_send(direction, k)
    send(tok.at[0, own_rows], tok.at[0, own_rows], tp_send, own_recv, partner)
    routes_all[0, core] = routes_t_ref[...]

    home_selection()
    await_copy(routes_all.at[0, other], rp_recv)
    await_copy(routes_all.at[1:RING], r_recv)
    source_slots()
    other_rows = pl.ds(pl.multiple_of(other * local_tokens, local_tokens), local_tokens)
    await_copy(tok.at[0, other_rows], own_recv)
    z_event(0)
    gather(0)
    y_event(0)
    z_event(1)
    partner_event(0)
    partner_event(1)
    gather(1)
    gather(2)
    z_event(2)
    y_event(1)
    z_event(3)
    partner_event(2)
    partner_event(3)
    gather(3)
    y_event(2)
    gather(4)
    z_event(4)
    x_event(0)
    x_event(1)
    z_event(5)
    y_event(3)
    multiply(0, 0, 5)
    send_back(0, (3, 4, 1, 2, 0))
    partner_event(4)
    partner_event(5)
    gather(5)
    gather(6)
    multiply(0, 5, 7)
    send_back(0, (5, 6))
    z_event(6)
    partner_event(6)
    gather(7)
    multiply(0, 7, 8)
    send_back(0, (7,))
    y_event(4)
    order = (7, 5, 6, 3, 4, 1, 2, 0)
    x_event(2)
    x_event(3)
    multiply(1, 0, 8)
    send_back(1, order)
    multiply(2, 0, 8)
    send_back(2, order)
    y_event(5)
    y_event(6)
    x_event(4)
    assemble(0)
    x_event(5)
    multiply(3, 0, 8)
    send_back(3, order)
    assemble(1)
    x_event(6)
    multiply(4, 0, 8)
    send_back(4, order)
    assemble(2)
    assemble(3)
    await_returned(4)
    await_copy(tok.at[0 : RING - 1, 0:local_tokens], tz_send)
    await_copy(tok.at[:, 0:local_tokens], tp_send)
    await_copy(wts.at[0 : RING - 1, 0 : hidden // 2], wy_send)
    await_copy(wts.at[0 : RING - 1, 0 : hidden // 2], wx_send)
    await_copy(routes_all.at[1:RING], r_send)
    await_copy(routes_all.at[0, other], rp_send)
    for group in range(len(GROUPS)):
        await_copy(outgoing[group].at[2 : 2 * RING], b_send.at[group])
        await_copy(outgoing[group].at[other], bp_send.at[group])


def finish_kernel(out_ref, returned_4, select_4, scale, final_ref, buffer, sems):
    f32, bf16 = jnp.float32, jnp.bfloat16
    hidden = returned_4.shape[-1]
    rows = buffer.shape[1]
    steps = buffer.shape[0]
    blocks = [returned_4[c].reshape(RING * CAP, hidden) for c in range(2)]
    copies = []
    for n in range(steps):
        span = slice(n * rows, (n + 1) * rows)
        factor = scale[span, :]
        for c in range(2):
            got = jnp.dot(select_4[span, :], blocks[c], preferred_element_type=f32)
            for col in range(0, hidden, 128):
                columns = slice(c * hidden + col, c * hidden + col + 128)
                term = (factor * got[:, col : col + 128]).astype(bf16)
                buffer[n, :, columns] = out_ref[span, columns] + term
        copies.append(pltpu.make_async_copy(buffer.at[n], final_ref.at[span], sems.at[n]))
        if n > 0:
            copies[n - 1].start()
    copies[-1].start()
    for copy in copies:
        copy.wait()


def shards(expert_down, out_grad, routes, gates):
    hidden, width = expert_down.shape
    local_tokens, top = routes.shape
    choices = local_tokens * top
    bf16 = jnp.bfloat16
    dma = pltpu.SemaphoreType.DMA
    vmem = pl.BlockSpec(memory_space=pltpu.VMEM)
    hbm = pl.BlockSpec(memory_space=pl.ANY)
    parts = pl.pallas_call(
        kernel,
        out_shape=(
            pltpu.VMEM((choices, 2 * hidden), bf16),
            pltpu.VMEM((2, RING, CAP, hidden), bf16),
            pltpu.VMEM((choices, RING * CAP), bf16),
            pltpu.VMEM((choices, 128), jnp.float32),
        ),
        in_specs=[hbm, hbm, vmem, vmem],
        out_specs=[vmem] * 4,
        scratch_shapes=[
            pltpu.VMEM((RING, 2 * local_tokens, width), bf16),
            pltpu.VMEM((RING, hidden, width), bf16),
            pltpu.VMEM((RING, RING * PAIR, width), bf16),
            *[pltpu.VMEM((2 * RING, len(g) * CAP, hidden), bf16) for g in GROUPS],
            *[pltpu.VMEM((2, RING, len(g) * CAP, hidden), bf16) for g in GROUPS[:-1]],
            pltpu.VMEM((choices, STARTS[-1]), bf16),
            pltpu.VMEM((RING, 2, top, local_tokens), jnp.int32),
            pltpu.VMEM((RING, 2, RING, local_tokens), jnp.float32),
            dma((2,)),
            dma(()),
            dma((2, 7)),
            dma(()),
            dma((2, 7)),
            dma(()),
            dma(()),
            dma((2, 7)),
            dma(()),
            dma((2, 7)),
            dma(()),
            dma(()),
            dma(()),
            dma(()),
            dma((len(GROUPS),)),
            dma((len(GROUPS),)),
            dma((len(GROUPS),)),
            dma((len(GROUPS),)),
        ],
        compiler_params=pltpu.CompilerParams(
            collective_id=0, has_side_effects=True, vmem_limit_bytes=52 * 2**20
        ),
    )(expert_down, out_grad, routes.T, gates.T)
    steps = 8
    final = pl.pallas_call(
        finish_kernel,
        out_shape=jax.ShapeDtypeStruct((choices, 2 * hidden), bf16),
        in_specs=[vmem] * 4,
        out_specs=hbm,
        scratch_shapes=[
            pltpu.VMEM((steps, choices // steps, 2 * hidden), bf16),
            dma((steps,)),
        ],
        compiler_params=pltpu.CompilerParams(vmem_limit_bytes=16 * 2**20),
    )(*parts)
    return final.reshape(local_tokens, top, 2 * hidden)


def solution(mesh):
    placed = (
        P("expert", None),
        P(("dp", "expert"), None),
        P(("dp", "expert"), None),
        P(("dp", "expert"), None),
    )
    return jax.shard_map(
        shards,
        mesh=mesh,
        in_specs=placed,
        out_specs=P(("dp", "expert"), None, None),
        check_vma=False,
    )
```

```python
import functools

import jax
import jax.numpy as jnp
from jax import lax
from jax.experimental import pallas as pl
from jax.experimental.pallas import tpu as pltpu
from jax.sharding import PartitionSpec as P

MESH = pl.DeviceIdType.MESH
RING = 8
X_RING = 4
CAP = 24
PAIR = 2 * CAP
REL = (0, 1, 7, 2, 6, 3, 5, 4)
POS = tuple(REL.index(rel) for rel in range(RING))
GROUPS = ((0, 1), (2, 3), (4,), (5, 6), (7,))
STARTS = tuple(sum(len(g) for g in GROUPS[:n]) * RING * CAP for n in range(len(GROUPS)))


def position_of(rel):
    return jnp.where(rel == 0, 0, jnp.where(rel <= 4, 2 * rel - 1, 2 * (8 - rel)))


def rel_of(position):
    half = (position + 1) >> 1
    return jnp.where(position & 1 == 1, half, (8 - half) & 7)


def kernel(
    down_ref,
    grad_ref,
    routes_t_ref,
    gates_t_ref,
    out_ref,
    returned_4,
    select_4,
    scale,
    tok,
    wts,
    rows_x,
    outgoing_0,
    outgoing_1,
    outgoing_2,
    outgoing_3,
    outgoing_4,
    returned_0,
    returned_1,
    returned_2,
    returned_3,
    select,
    routes_all,
    slots_all,
    local_sem,
    tz_send,
    tz_recv,
    tp_send,
    tp_recv,
    own_recv,
    wy_send,
    wy_recv,
    wx_send,
    wx_recv,
    r_send,
    r_recv,
    rp_send,
    rp_recv,
    b_send,
    b_recv,
    bp_send,
    bp_recv,
):
    f32, bf16 = jnp.float32, jnp.bfloat16
    outgoing = (outgoing_0, outgoing_1, outgoing_2, outgoing_3, outgoing_4)
    returned = (returned_0, returned_1, returned_2, returned_3, returned_4)
    local_tokens, width = grad_ref.shape
    hidden = down_ref.shape[0]
    half_tok = local_tokens // 2
    quarter = hidden // 4
    x = lax.axis_index("dp")
    ex = lax.axis_index("expert")
    core = ex % 2
    other = 1 - core
    y = (ex // 2) % RING
    z = ex // (2 * RING)

    def at_z(rel, c):
        return (x, (((z + rel) % RING) * RING + y) * 2 + c)

    def at_y(rel):
        return (x, (z * RING + (y + rel) % RING) * 2 + core)

    def at_x(rel):
        return ((x + rel) % X_RING, ex)

    partner = (x, ex + 1 - 2 * core)

    def send(src, dst, send_sem, recv_sem, device):
        copy = pltpu.make_async_remote_copy(
            src_ref=src,
            dst_ref=dst,
            send_sem=send_sem,
            recv_sem=recv_sem,
            device_id=device,
            device_id_type=MESH,
        )
        copy.start()

    def await_copy(ref, sem):
        pltpu.make_async_copy(ref, ref, sem).wait()

    own_rows = pl.ds(pl.multiple_of(core * local_tokens, local_tokens), local_tokens)
    load_tok = pltpu.make_async_copy(grad_ref, tok.at[0, own_rows], local_sem.at[0])
    load_wts = pltpu.make_async_copy(down_ref, wts.at[0], local_sem.at[1])
    load_tok.start()
    load_wts.start()

    barrier = pltpu.get_barrier_semaphore()
    peers = [partner, at_y(1), at_y(-1 + RING), at_x(1), at_x(-1 + X_RING)]
    peers += [at_z(rel, c) for rel in range(1, RING) for c in range(2)]
    for peer in peers:
        pl.semaphore_signal(barrier, inc=1, device_id=peer, device_id_type=MESH)
    pl.semaphore_wait(barrier, len(peers))

    def tok_chunk(rel, half, c=None):
        c = core if c is None else c
        start = pl.multiple_of(c * local_tokens + half * half_tok, half_tok)
        return tok.at[POS[rel % RING], pl.ds(start, half_tok)]

    def z_send(direction, k):
        d = k // 2
        if direction == 0:
            half, src, dst, hop = k % 2, -d, -d - 1, 1
        else:
            half, src, dst, hop = 1 - k % 2, d, d + 1, RING - 1
        send(
            tok_chunk(src, half),
            tok_chunk(dst, half),
            tz_send,
            tz_recv.at[direction, k],
            at_z(hop, core),
        )

    def z_arrival(direction, k):
        d = k // 2
        return (-d - 1, k % 2) if direction == 0 else (d + 1, 1 - k % 2)

    def z_event(k):
        for direction in range(2):
            chunk = z_arrival(direction, k)
            await_copy(tok_chunk(*chunk), tz_recv.at[direction, k])
            if k <= 4:
                z_send(direction, k + 2)
            send(
                tok_chunk(*chunk),
                tok_chunk(*chunk),
                tp_send,
                tp_recv.at[direction, k],
                partner,
            )

    def partner_event(k):
        for direction in range(2):
            await_copy(tok_chunk(*z_arrival(direction, k), other), tp_recv.at[direction, k])

    base = 2 * (x % 2)

    def w_chunk(rel, part, quarters):
        start = pl.multiple_of((quarters + part) * quarter, quarter)
        return wts.at[POS[rel % RING], pl.ds(start, quarter)]

    def y_send(direction, k):
        d = k // 2
        if direction == 0:
            part, src, dst, hop = k % 2, -d, -d - 1, 1
        else:
            part, src, dst, hop = 1 - k % 2, d, d + 1, RING - 1
        send(
            w_chunk(src, part, base),
            w_chunk(dst, part, base),
            wy_send,
            wy_recv.at[direction, k],
            at_y(hop),
        )

    def y_event(k):
        for direction in range(2):
            rel, part = z_arrival(direction, k)
            await_copy(w_chunk(rel, part, base), wy_recv.at[direction, k])
            if k <= 4:
                y_send(direction, k + 2)
            send(
                w_chunk(rel, part, base),
                w_chunk(rel, part, base),
                wx_send,
                wx_recv.at[part, k],
                at_x(X_RING - 1 if part == 0 else 1),
            )

    def x_event(k):
        for direction in range(2):
            rel, part = z_arrival(direction, k)
            await_copy(w_chunk(rel, part, 2 - base), wx_recv.at[part, k])

    def gather(q):
        slots = jnp.concatenate([slots_all[q, 0], slots_all[q, 1]], axis=1)
        number = lax.broadcasted_iota(jnp.int32, (PAIR, 2 * local_tokens), 0).astype(f32)
        pick = jnp.concatenate(
            [jnp.where(slots[p : p + 1, :] == number, 1.0, 0.0) for p in range(RING)], axis=0
        ).astype(bf16)
        cols = 512

        def body(n, carry):
            span = pl.ds(pl.multiple_of(n * cols, cols), cols)
            got = jnp.dot(pick, tok[q, :, span], preferred_element_type=f32)
            rows_x[:, q * PAIR : (q + 1) * PAIR, span] = got.astype(bf16).reshape(RING, PAIR, cols)
            return carry

        lax.fori_loop(0, width // cols, body, 0)

    def multiply(group, first, last):
        products = []
        for p in GROUPS[group]:
            value = lax.dot_general(
                rows_x[p, first * PAIR : last * PAIR, :],
                wts[p],
                (((1,), (1,)), ((), ())),
                preferred_element_type=f32,
            )
            products.append(value.reshape(2 * (last - first), CAP, hidden))
        both = jnp.concatenate(products, axis=1) if len(products) > 1 else products[0]
        outgoing[group][2 * first : 2 * last] = both.astype(bf16)

    def keep_own(group):
        returned[group][core, 0] = outgoing[group][core]

    def send_in_z_order(group):
        for dest in range(RING):
            rel = (dest - z + RING) % RING

            @pl.when(rel != 0)
            def _():
                for c in range(2):
                    send(
                        outgoing[group].at[2 * position_of(rel) + c],
                        returned[group].at[core, position_of((RING - rel) % RING)],
                        b_send.at[group],
                        b_recv.at[group],
                        at_z(rel, c),
                    )

    def send_back(group, positions):
        for q in positions:
            rel = REL[q]
            if q == 0:
                send(
                    outgoing[group].at[other],
                    returned[group].at[core, 0],
                    bp_send.at[group],
                    bp_recv.at[group],
                    partner,
                )
                continue
            for c in range(2):
                send(
                    outgoing[group].at[2 * q + c],
                    returned[group].at[core, POS[(RING - rel) % RING]],
                    b_send.at[group],
                    b_recv.at[group],
                    at_z(rel, c),
                )

    def await_returned(group):
        await_copy(returned[group].at[other, 0], bp_recv.at[group])
        await_copy(returned[group].at[:, 1:RING], b_recv.at[group])

    def assemble(group):
        await_returned(group)
        rows = 4 * local_tokens
        depth = len(GROUPS[group]) * RING * CAP

        for c in range(2):

            def body(n, carry):
                span = pl.ds(pl.multiple_of(n * rows, rows), rows)
                got = jnp.dot(
                    select[span, STARTS[group] : STARTS[group] + depth],
                    returned[group][c].reshape(depth, hidden),
                    preferred_element_type=f32,
                )
                factor = scale[span, :]
                for col in range(0, hidden, 128):
                    columns = slice(c * hidden + col, c * hidden + col + 128)
                    term = (factor * got[:, col : col + 128]).astype(bf16)
                    if group == 0:
                        out_ref[span, columns] = term
                    else:
                        out_ref[span, columns] = out_ref[span, columns] + term
                return carry

            lax.fori_loop(0, out_ref.shape[0] // rows, body, 0)

    def home_selection():
        top = routes_t_ref.shape[0]
        routes = routes_t_ref[...]
        lane = lax.broadcasted_iota(jnp.int32, (local_tokens, local_tokens), 1)
        sub = lax.broadcasted_iota(jnp.int32, (local_tokens, local_tokens), 0)
        expert_by_token = jnp.zeros((local_tokens, local_tokens), f32)
        for j in range(top):
            expert_by_token = jnp.where(routes[j : j + 1, :] == sub, 1.0, expert_by_token)
        earlier = jnp.where(lane < sub, 1.0, 0.0).astype(bf16)
        counts = lax.dot_general(
            earlier,
            expert_by_token.astype(bf16),
            (((1,), (1,)), ((), ())),
            preferred_element_type=f32,
        ).astype(bf16)
        p = position_of(((lane & 7) - y + RING) & 7)
        q = position_of(((lane >> 3) - z + 2 * RING) & 7)
        first = jnp.zeros(lane.shape, jnp.int32)
        for start, group in zip(STARTS, GROUPS):
            for n, member in enumerate(group):
                row = start + q * (len(group) * CAP) + n * CAP
                first = jnp.where(p == member, row, first)
        first = first.astype(f32)
        lane_f = lane.astype(f32)
        columns = RING * PAIR
        number = lax.broadcasted_iota(jnp.int32, (local_tokens, columns), 1).astype(f32)
        per_step = local_tokens // top
        routes_rows = jnp.concatenate([routes.astype(f32)] * per_step, axis=0)
        gates_rows = jnp.concatenate([gates_t_ref[...]] * per_step, axis=0)

        def body(n, carry):
            here = n * per_step + (sub >> 3) == lane
            repeat = jnp.where(here, 1.0, 0.0).astype(bf16)
            chosen = jnp.sum(jnp.where(here, routes_rows, 0.0), axis=1, keepdims=True)
            gate = jnp.sum(jnp.where(here, gates_rows, 0.0), axis=1, keepdims=True)
            slot = jnp.dot(repeat, counts, preferred_element_type=f32)
            place = jnp.sum(jnp.where(lane_f == chosen, slot + first, 0.0), axis=1, keepdims=True)
            span = pl.ds(pl.multiple_of(n * local_tokens, local_tokens), local_tokens)
            scale[span, :] = jnp.broadcast_to(gate, (local_tokens, scale.shape[1]))
            for start in range(0, STARTS[-1], columns):
                size = min(columns, STARTS[-1] - start)
                hit = jnp.where(place == number[:, :size] + float(start), 1.0, 0.0)
                select[span, start : start + size] = hit.astype(bf16)
            last = jnp.where(place == number[:, : select_4.shape[1]] + float(STARTS[-1]), 1.0, 0.0)
            select_4[span, :] = last.astype(bf16)
            return carry

        lax.fori_loop(0, top, body, 0)

    def source_slots():
        sub = lax.broadcasted_iota(jnp.int32, (RING, local_tokens), 0)
        expert = z * RING + ((y + rel_of(sub)) & 7)
        named = []
        for q in range(RING):
            for s in range(2):
                value = jnp.zeros((RING, local_tokens), f32)
                for j in range(RING):
                    value = jnp.where(routes_all[q, s, j : j + 1, :] == expert, 1.0, value)
                named.append(value)
        named = jnp.concatenate(named, axis=0)
        a = lax.broadcasted_iota(jnp.int32, (local_tokens, local_tokens), 0)
        b = lax.broadcasted_iota(jnp.int32, (local_tokens, local_tokens), 1)
        before = jnp.where(a < b, 1.0, 0.0).astype(bf16)
        counts = jnp.dot(named.astype(bf16), before, preferred_element_type=f32)
        row = lax.broadcasted_iota(jnp.int32, named.shape, 0)
        counts = counts + jnp.where((row >> 3) & 1 == 1, float(CAP), 0.0)
        slots_all[...] = jnp.where(named > 0.5, counts, -1.0).reshape(slots_all.shape)

    for rel in (4, 3, 5, 2, 6, 1, 7):
        for c in range(2):
            send(
                routes_t_ref,
                routes_all.at[POS[RING - rel], core],
                r_send,
                r_recv,
                at_z(rel, c),
            )
    send(routes_t_ref, routes_all.at[0, core], rp_send, rp_recv, partner)
    load_tok.wait()
    for k in range(2):
        for direction in range(2):
            z_send(direction, k)
    load_wts.wait()
    for k in range(2):
        for direction in range(2):
            y_send(direction, k)
    send(tok.at[0, own_rows], tok.at[0, own_rows], tp_send, own_recv, partner)
    routes_all[0, core] = routes_t_ref[...]

    home_selection()
    await_copy(routes_all.at[0, other], rp_recv)
    await_copy(routes_all.at[1:RING], r_recv)
    source_slots()
    other_rows = pl.ds(pl.multiple_of(other * local_tokens, local_tokens), local_tokens)
    await_copy(tok.at[0, other_rows], own_recv)
    z_event(0)
    gather(0)
    y_event(0)
    z_event(1)
    partner_event(0)
    partner_event(1)
    gather(1)
    gather(2)
    z_event(2)
    y_event(1)
    z_event(3)
    partner_event(2)
    partner_event(3)
    gather(3)
    y_event(2)
    gather(4)
    z_event(4)
    x_event(0)
    x_event(1)
    z_event(5)
    y_event(3)
    multiply(0, 0, 5)
    keep_own(0)
    send_back(0, (3, 4, 1, 2, 0))
    partner_event(4)
    partner_event(5)
    gather(5)
    gather(6)
    multiply(0, 5, 7)
    send_back(0, (5, 6))
    z_event(6)
    partner_event(6)
    gather(7)
    multiply(0, 7, 8)
    send_back(0, (7,))
    y_event(4)
    order = (7, 5, 6, 3, 4, 1, 2, 0)
    x_event(2)
    x_event(3)
    multiply(1, 0, 8)
    keep_own(1)
    send_back(1, order)
    multiply(2, 0, 8)
    keep_own(2)
    send_back(2, order)
    y_event(5)
    y_event(6)
    x_event(4)
    assemble(0)
    x_event(5)
    multiply(3, 0, 8)
    keep_own(3)
    send_back(3, order)
    assemble(1)
    x_event(6)
    multiply(4, 0, 8)
    keep_own(4)
    send_in_z_order(4)
    send_back(4, (0,))
    assemble(2)
    assemble(3)
    await_returned(4)
    await_copy(tok.at[0 : RING - 1, 0:local_tokens], tz_send)
    await_copy(tok.at[:, 0:local_tokens], tp_send)
    await_copy(wts.at[0 : RING - 1, 0 : hidden // 2], wy_send)
    await_copy(wts.at[0 : RING - 1, 0 : hidden // 2], wx_send)
    await_copy(routes_all.at[1:RING], r_send)
    await_copy(routes_all.at[0, other], rp_send)
    for group in range(len(GROUPS)):
        await_copy(outgoing[group].at[2 : 2 * RING], b_send.at[group])
        await_copy(outgoing[group].at[other], bp_send.at[group])


def finish_kernel(out_ref, returned_4, select_4, scale, final_ref, buffer, sems):
    f32, bf16 = jnp.float32, jnp.bfloat16
    hidden = returned_4.shape[-1]
    rows = buffer.shape[1]
    steps = buffer.shape[0]
    blocks = [returned_4[c].reshape(RING * CAP, hidden) for c in range(2)]
    copies = []
    for n in range(steps):
        span = slice(n * rows, (n + 1) * rows)
        factor = scale[span, :]
        for c in range(2):
            got = jnp.dot(select_4[span, :], blocks[c], preferred_element_type=f32)
            for col in range(0, hidden, 128):
                columns = slice(c * hidden + col, c * hidden + col + 128)
                term = (factor * got[:, col : col + 128]).astype(bf16)
                buffer[n, :, columns] = out_ref[span, columns] + term
        copies.append(pltpu.make_async_copy(buffer.at[n], final_ref.at[span], sems.at[n]))
        if n > 0:
            copies[n - 1].start()
    copies[-1].start()
    for copy in copies:
        copy.wait()


def shards(expert_down, out_grad, routes, gates):
    hidden, width = expert_down.shape
    local_tokens, top = routes.shape
    choices = local_tokens * top
    bf16 = jnp.bfloat16
    dma = pltpu.SemaphoreType.DMA
    vmem = pl.BlockSpec(memory_space=pltpu.VMEM)
    hbm = pl.BlockSpec(memory_space=pl.ANY)
    parts = pl.pallas_call(
        kernel,
        out_shape=(
            pltpu.VMEM((choices, 2 * hidden), bf16),
            pltpu.VMEM((2, RING, CAP, hidden), bf16),
            pltpu.VMEM((choices, RING * CAP), bf16),
            pltpu.VMEM((choices, 128), jnp.float32),
        ),
        in_specs=[hbm, hbm, vmem, vmem],
        out_specs=[vmem] * 4,
        scratch_shapes=[
            pltpu.VMEM((RING, 2 * local_tokens, width), bf16),
            pltpu.VMEM((RING, hidden, width), bf16),
            pltpu.VMEM((RING, RING * PAIR, width), bf16),
            *[pltpu.VMEM((2 * RING, len(g) * CAP, hidden), bf16) for g in GROUPS],
            *[pltpu.VMEM((2, RING, len(g) * CAP, hidden), bf16) for g in GROUPS[:-1]],
            pltpu.VMEM((choices, STARTS[-1]), bf16),
            pltpu.VMEM((RING, 2, top, local_tokens), jnp.int32),
            pltpu.VMEM((RING, 2, RING, local_tokens), jnp.float32),
            dma((2,)),
            dma(()),
            dma((2, 7)),
            dma(()),
            dma((2, 7)),
            dma(()),
            dma(()),
            dma((2, 7)),
            dma(()),
            dma((2, 7)),
            dma(()),
            dma(()),
            dma(()),
            dma(()),
            dma((len(GROUPS),)),
            dma((len(GROUPS),)),
            dma((len(GROUPS),)),
            dma((len(GROUPS),)),
        ],
        compiler_params=pltpu.CompilerParams(
            collective_id=0, has_side_effects=True, vmem_limit_bytes=52 * 2**20
        ),
    )(expert_down, out_grad, routes.T, gates.T)
    steps = 8
    final = pl.pallas_call(
        finish_kernel,
        out_shape=jax.ShapeDtypeStruct((choices, 2 * hidden), bf16),
        in_specs=[vmem] * 4,
        out_specs=hbm,
        scratch_shapes=[
            pltpu.VMEM((steps, choices // steps, 2 * hidden), bf16),
            dma((steps,)),
        ],
        compiler_params=pltpu.CompilerParams(vmem_limit_bytes=16 * 2**20),
    )(*parts)
    return final.reshape(local_tokens, top, 2 * hidden)


def solution(mesh):
    placed = (
        P("expert", None),
        P(("dp", "expert"), None),
        P(("dp", "expert"), None),
        P(("dp", "expert"), None),
    )
    return jax.shard_map(
        shards,
        mesh=mesh,
        in_specs=placed,
        out_specs=P(("dp", "expert"), None, None),
        check_vma=False,
    )
```

```python
import functools

import jax
import jax.numpy as jnp
from jax import lax
from jax.experimental import pallas as pl
from jax.experimental.pallas import tpu as pltpu
from jax.sharding import PartitionSpec as P

MESH = pl.DeviceIdType.MESH
RING = 8
X_RING = 4
CAP = 24
PAIR = 2 * CAP
REL = (0, 1, 7, 2, 6, 3, 5, 4)
POS = tuple(REL.index(rel) for rel in range(RING))
GROUPS = ((0, 1), (2, 3), (4,), (5, 6), (7,))
STARTS = tuple(sum(len(g) for g in GROUPS[:n]) * RING * CAP for n in range(len(GROUPS)))


def position_of(rel):
    return jnp.where(rel == 0, 0, jnp.where(rel <= 4, 2 * rel - 1, 2 * (8 - rel)))


def rel_of(position):
    half = (position + 1) >> 1
    return jnp.where(position & 1 == 1, half, (8 - half) & 7)


def kernel(
    down_ref,
    grad_ref,
    routes_t_ref,
    gates_t_ref,
    out_ref,
    returned_4,
    select_4,
    scale,
    tok,
    wts,
    rows_x,
    outgoing_0,
    outgoing_1,
    outgoing_2,
    outgoing_3,
    outgoing_4,
    returned_0,
    returned_1,
    returned_2,
    returned_3,
    select,
    routes_all,
    slots_all,
    local_sem,
    tz_send,
    tz_recv,
    tp_send,
    tp_recv,
    own_recv,
    wy_send,
    wy_recv,
    wx_send,
    wx_recv,
    r_send,
    r_recv,
    rp_send,
    rp_recv,
    b_send,
    b_recv,
    bp_send,
    bp_recv,
):
    f32, bf16 = jnp.float32, jnp.bfloat16
    outgoing = (outgoing_0, outgoing_1, outgoing_2, outgoing_3, outgoing_4)
    returned = (returned_0, returned_1, returned_2, returned_3, returned_4)
    local_tokens, width = grad_ref.shape
    hidden = down_ref.shape[0]
    half_tok = local_tokens // 2
    quarter = hidden // 4
    x = lax.axis_index("dp")
    ex = lax.axis_index("expert")
    core = ex % 2
    other = 1 - core
    y = (ex // 2) % RING
    z = ex // (2 * RING)

    def at_z(rel, c):
        return (x, (((z + rel) % RING) * RING + y) * 2 + c)

    def at_y(rel):
        return (x, (z * RING + (y + rel) % RING) * 2 + core)

    def at_x(rel):
        return ((x + rel) % X_RING, ex)

    partner = (x, ex + 1 - 2 * core)

    def send(src, dst, send_sem, recv_sem, device):
        copy = pltpu.make_async_remote_copy(
            src_ref=src,
            dst_ref=dst,
            send_sem=send_sem,
            recv_sem=recv_sem,
            device_id=device,
            device_id_type=MESH,
        )
        copy.start()

    def await_copy(ref, sem):
        pltpu.make_async_copy(ref, ref, sem).wait()

    own_rows = pl.ds(pl.multiple_of(core * local_tokens, local_tokens), local_tokens)
    load_tok = pltpu.make_async_copy(grad_ref, tok.at[0, own_rows], local_sem.at[0])
    load_wts = pltpu.make_async_copy(down_ref, wts.at[0], local_sem.at[1])
    load_tok.start()
    load_wts.start()

    barrier = pltpu.get_barrier_semaphore()
    peers = [partner, at_y(1), at_y(RING - 1), at_x(1), at_x(X_RING - 1)]
    peers += [at_z(1, core), at_z(RING - 1, core)]
    for peer in peers:
        pl.semaphore_signal(barrier, inc=1, device_id=peer, device_id_type=MESH)
    pl.semaphore_wait(barrier, len(peers))

    def tok_chunk(rel, half, c=None):
        c = core if c is None else c
        start = pl.multiple_of(c * local_tokens + half * half_tok, half_tok)
        return tok.at[POS[rel % RING], pl.ds(start, half_tok)]

    def z_send(direction, k):
        d = k // 2
        if direction == 0:
            half, src, dst, hop = k % 2, -d, -d - 1, 1
        else:
            half, src, dst, hop = 1 - k % 2, d, d + 1, RING - 1
        send(
            tok_chunk(src, half),
            tok_chunk(dst, half),
            tz_send,
            tz_recv.at[direction, k],
            at_z(hop, core),
        )

    def routes_send(direction, d):
        src, dst, hop = (-d, -d - 1, 1) if direction == 0 else (d, d + 1, RING - 1)
        send(
            routes_all.at[POS[src % RING], core] if d else routes_t_ref,
            routes_all.at[POS[dst % RING], core],
            r_send,
            r_recv.at[direction, d],
            at_z(hop, core),
        )

    def z_arrival(direction, k):
        d = k // 2
        return (-d - 1, k % 2) if direction == 0 else (d + 1, 1 - k % 2)

    def z_event(k):
        for direction in range(2):
            chunk = z_arrival(direction, k)
            d = k // 2
            if k % 2 == 0 and d + direction < 4:
                spot = POS[chunk[0] % RING]
                await_copy(routes_all.at[spot, core], r_recv.at[direction, d])
                if d + 1 + direction < 4:
                    routes_send(direction, d + 1)
                send(
                    routes_all.at[spot, core],
                    routes_all.at[spot, core],
                    rp_send,
                    rp_recv.at[direction, d],
                    partner,
                )
            await_copy(tok_chunk(*chunk), tz_recv.at[direction, k])
            if k <= 4:
                z_send(direction, k + 2)
            send(
                tok_chunk(*chunk),
                tok_chunk(*chunk),
                tp_send,
                tp_recv.at[direction, k],
                partner,
            )

    def partner_event(k):
        for direction in range(2):
            rel, half = z_arrival(direction, k)
            if k % 2 == 0 and k // 2 + direction < 4:
                await_copy(routes_all.at[POS[rel % RING], other], rp_recv.at[direction, k // 2])
            await_copy(tok_chunk(rel, half, other), tp_recv.at[direction, k])

    base = 2 * (x % 2)

    def w_chunk(rel, part, quarters):
        start = pl.multiple_of((quarters + part) * quarter, quarter)
        return wts.at[POS[rel % RING], pl.ds(start, quarter)]

    def y_send(direction, k):
        d = k // 2
        if direction == 0:
            part, src, dst, hop = k % 2, -d, -d - 1, 1
        else:
            part, src, dst, hop = 1 - k % 2, d, d + 1, RING - 1
        send(
            w_chunk(src, part, base),
            w_chunk(dst, part, base),
            wy_send,
            wy_recv.at[direction, k],
            at_y(hop),
        )

    def y_event(k):
        for direction in range(2):
            rel, part = z_arrival(direction, k)
            await_copy(w_chunk(rel, part, base), wy_recv.at[direction, k])
            if k <= 4:
                y_send(direction, k + 2)
            send(
                w_chunk(rel, part, base),
                w_chunk(rel, part, base),
                wx_send,
                wx_recv.at[part, k],
                at_x(X_RING - 1 if part == 0 else 1),
            )

    def x_event(k):
        for direction in range(2):
            rel, part = z_arrival(direction, k)
            await_copy(w_chunk(rel, part, 2 - base), wx_recv.at[part, k])

    def gather(q):
        slots = jnp.concatenate([slots_all[q, 0], slots_all[q, 1]], axis=1)
        number = lax.broadcasted_iota(jnp.int32, (PAIR, 2 * local_tokens), 0).astype(f32)
        pick = jnp.concatenate(
            [jnp.where(slots[p : p + 1, :] == number, 1.0, 0.0) for p in range(RING)], axis=0
        ).astype(bf16)
        cols = 512

        def body(n, carry):
            span = pl.ds(pl.multiple_of(n * cols, cols), cols)
            got = jnp.dot(pick, tok[q, :, span], preferred_element_type=f32)
            rows_x[:, q * PAIR : (q + 1) * PAIR, span] = got.astype(bf16).reshape(RING, PAIR, cols)
            return carry

        lax.fori_loop(0, width // cols, body, 0)

    def multiply(group, first, last):
        products = []
        for p in GROUPS[group]:
            value = lax.dot_general(
                rows_x[p, first * PAIR : last * PAIR, :],
                wts[p],
                (((1,), (1,)), ((), ())),
                preferred_element_type=f32,
            )
            products.append(value.reshape(2 * (last - first), CAP, hidden))
        both = jnp.concatenate(products, axis=1) if len(products) > 1 else products[0]
        outgoing[group][2 * first : 2 * last] = both.astype(bf16)

    def keep_own(group):
        returned[group][core, 0] = outgoing[group][core]

    def send_in_z_order(group):
        for dest in range(RING):
            rel = (dest - z + RING) % RING

            @pl.when(rel != 0)
            def _():
                for c in range(2):
                    send(
                        outgoing[group].at[2 * position_of(rel) + c],
                        returned[group].at[core, position_of((RING - rel) % RING)],
                        b_send.at[group],
                        b_recv.at[group],
                        at_z(rel, c),
                    )

    def send_back(group, positions):
        for q in positions:
            rel = REL[q]
            if q == 0:
                send(
                    outgoing[group].at[other],
                    returned[group].at[core, 0],
                    bp_send.at[group],
                    bp_recv.at[group],
                    partner,
                )
                continue
            for c in range(2):
                send(
                    outgoing[group].at[2 * q + c],
                    returned[group].at[core, POS[(RING - rel) % RING]],
                    b_send.at[group],
                    b_recv.at[group],
                    at_z(rel, c),
                )

    def await_returned(group):
        await_copy(returned[group].at[other, 0], bp_recv.at[group])
        await_copy(returned[group].at[:, 1:RING], b_recv.at[group])

    def assemble(group):
        await_returned(group)
        rows = 4 * local_tokens
        depth = len(GROUPS[group]) * RING * CAP

        for c in range(2):

            def body(n, carry):
                span = pl.ds(pl.multiple_of(n * rows, rows), rows)
                got = jnp.dot(
                    select[span, STARTS[group] : STARTS[group] + depth],
                    returned[group][c].reshape(depth, hidden),
                    preferred_element_type=f32,
                )
                factor = scale[span, :]
                for col in range(0, hidden, 128):
                    columns = slice(c * hidden + col, c * hidden + col + 128)
                    term = (factor * got[:, col : col + 128]).astype(bf16)
                    if group == 0:
                        out_ref[span, columns] = term
                    else:
                        out_ref[span, columns] = out_ref[span, columns] + term
                return carry

            lax.fori_loop(0, out_ref.shape[0] // rows, body, 0)

    def home_selection():
        top = routes_t_ref.shape[0]
        routes = routes_t_ref[...]
        lane = lax.broadcasted_iota(jnp.int32, (local_tokens, local_tokens), 1)
        sub = lax.broadcasted_iota(jnp.int32, (local_tokens, local_tokens), 0)
        expert_by_token = jnp.zeros((local_tokens, local_tokens), f32)
        for j in range(top):
            expert_by_token = jnp.where(routes[j : j + 1, :] == sub, 1.0, expert_by_token)
        earlier = jnp.where(lane < sub, 1.0, 0.0).astype(bf16)
        counts = lax.dot_general(
            earlier,
            expert_by_token.astype(bf16),
            (((1,), (1,)), ((), ())),
            preferred_element_type=f32,
        ).astype(bf16)
        p = position_of(((lane & 7) - y + RING) & 7)
        q = position_of(((lane >> 3) - z + 2 * RING) & 7)
        first = jnp.zeros(lane.shape, jnp.int32)
        for start, group in zip(STARTS, GROUPS):
            for n, member in enumerate(group):
                row = start + q * (len(group) * CAP) + n * CAP
                first = jnp.where(p == member, row, first)
        first = first.astype(f32)
        lane_f = lane.astype(f32)
        columns = RING * PAIR
        number = lax.broadcasted_iota(jnp.int32, (local_tokens, columns), 1).astype(f32)
        per_step = local_tokens // top
        routes_rows = jnp.concatenate([routes.astype(f32)] * per_step, axis=0)
        gates_rows = jnp.concatenate([gates_t_ref[...]] * per_step, axis=0)

        def body(n, carry):
            here = n * per_step + (sub >> 3) == lane
            repeat = jnp.where(here, 1.0, 0.0).astype(bf16)
            chosen = jnp.sum(jnp.where(here, routes_rows, 0.0), axis=1, keepdims=True)
            gate = jnp.sum(jnp.where(here, gates_rows, 0.0), axis=1, keepdims=True)
            slot = jnp.dot(repeat, counts, preferred_element_type=f32)
            place = jnp.sum(jnp.where(lane_f == chosen, slot + first, 0.0), axis=1, keepdims=True)
            span = pl.ds(pl.multiple_of(n * local_tokens, local_tokens), local_tokens)
            scale[span, :] = jnp.broadcast_to(gate, (local_tokens, scale.shape[1]))
            for start in range(0, STARTS[-1], columns):
                size = min(columns, STARTS[-1] - start)
                hit = jnp.where(place == number[:, :size] + float(start), 1.0, 0.0)
                select[span, start : start + size] = hit.astype(bf16)
            last = jnp.where(place == number[:, : select_4.shape[1]] + float(STARTS[-1]), 1.0, 0.0)
            select_4[span, :] = last.astype(bf16)
            return carry

        lax.fori_loop(0, top, body, 0)

    def source_slots(q):
        sub = lax.broadcasted_iota(jnp.int32, (RING, local_tokens), 0)
        expert = z * RING + ((y + rel_of(sub)) & 7)
        named = []
        for s in range(2):
            value = jnp.zeros((RING, local_tokens), f32)
            for j in range(RING):
                value = jnp.where(routes_all[q, s, j : j + 1, :] == expert, 1.0, value)
            named.append(value)
        named = jnp.concatenate(named, axis=0)
        a = lax.broadcasted_iota(jnp.int32, (local_tokens, local_tokens), 0)
        b = lax.broadcasted_iota(jnp.int32, (local_tokens, local_tokens), 1)
        before = jnp.where(a < b, 1.0, 0.0).astype(bf16)
        counts = jnp.dot(named.astype(bf16), before, preferred_element_type=f32)
        row = lax.broadcasted_iota(jnp.int32, named.shape, 0)
        counts = counts + jnp.where(row >= RING, float(CAP), 0.0)
        slots_all[q] = jnp.where(named > 0.5, counts, -1.0).reshape(slots_all.shape[1:])

    load_tok.wait()
    for direction in range(2):
        routes_send(direction, 0)
    for k in range(2):
        for direction in range(2):
            z_send(direction, k)
    send(routes_t_ref, routes_all.at[0, core], rp_send, own_recv.at[0], partner)
    load_wts.wait()
    for k in range(2):
        for direction in range(2):
            y_send(direction, k)
    send(tok.at[0, own_rows], tok.at[0, own_rows], tp_send, own_recv.at[1], partner)
    routes_all[0, core] = routes_t_ref[...]

    home_selection()
    await_copy(routes_all.at[0, other], own_recv.at[0])
    other_rows = pl.ds(pl.multiple_of(other * local_tokens, local_tokens), local_tokens)
    await_copy(tok.at[0, other_rows], own_recv.at[1])
    source_slots(0)
    z_event(0)
    gather(0)
    y_event(0)
    z_event(1)
    partner_event(0)
    partner_event(1)
    source_slots(1)
    gather(1)
    source_slots(2)
    gather(2)
    z_event(2)
    y_event(1)
    z_event(3)
    partner_event(2)
    partner_event(3)
    source_slots(3)
    gather(3)
    y_event(2)
    source_slots(4)
    gather(4)
    z_event(4)
    x_event(0)
    x_event(1)
    z_event(5)
    y_event(3)
    multiply(0, 0, 5)
    keep_own(0)
    send_back(0, (3, 4, 1, 2, 0))
    partner_event(4)
    partner_event(5)
    source_slots(5)
    gather(5)
    source_slots(6)
    gather(6)
    multiply(0, 5, 7)
    send_back(0, (5, 6))
    z_event(6)
    partner_event(6)
    source_slots(7)
    gather(7)
    multiply(0, 7, 8)
    send_back(0, (7,))
    y_event(4)
    order = (7, 5, 6, 3, 4, 1, 2, 0)
    x_event(2)
    x_event(3)
    multiply(1, 0, 8)
    keep_own(1)
    send_back(1, order)
    multiply(2, 0, 8)
    keep_own(2)
    send_back(2, order)
    y_event(5)
    y_event(6)
    x_event(4)
    assemble(0)
    x_event(5)
    multiply(3, 0, 8)
    keep_own(3)
    send_back(3, order)
    assemble(1)
    x_event(6)
    multiply(4, 0, 8)
    keep_own(4)
    send_in_z_order(4)
    send_back(4, (0,))
    assemble(2)
    assemble(3)
    await_returned(4)
    await_copy(tok.at[0 : RING - 1, 0:local_tokens], tz_send)
    await_copy(tok.at[:, 0:local_tokens], tp_send)
    await_copy(wts.at[0 : RING - 1, 0 : hidden // 2], wy_send)
    await_copy(wts.at[0 : RING - 1, 0 : hidden // 2], wx_send)
    await_copy(routes_all.at[0 : RING - 1, 0], r_send)
    await_copy(routes_all.at[:, 0], rp_send)
    for group in range(len(GROUPS)):
        await_copy(outgoing[group].at[2 : 2 * RING], b_send.at[group])
        await_copy(outgoing[group].at[other], bp_send.at[group])


def finish_kernel(out_ref, returned_4, select_4, scale, final_ref, buffer, sems):
    f32, bf16 = jnp.float32, jnp.bfloat16
    hidden = returned_4.shape[-1]
    rows = buffer.shape[1]
    steps = buffer.shape[0]
    blocks = [returned_4[c].reshape(RING * CAP, hidden) for c in range(2)]
    copies = []
    for n in range(steps):
        span = slice(n * rows, (n + 1) * rows)
        factor = scale[span, :]
        for c in range(2):
            got = jnp.dot(select_4[span, :], blocks[c], preferred_element_type=f32)
            for col in range(0, hidden, 128):
                columns = slice(c * hidden + col, c * hidden + col + 128)
                term = (factor * got[:, col : col + 128]).astype(bf16)
                buffer[n, :, columns] = out_ref[span, columns] + term
        copies.append(pltpu.make_async_copy(buffer.at[n], final_ref.at[span], sems.at[n]))
        if n > 0:
            copies[n - 1].start()
    copies[-1].start()
    for copy in copies:
        copy.wait()


def shards(expert_down, out_grad, routes, gates):
    hidden, width = expert_down.shape
    local_tokens, top = routes.shape
    choices = local_tokens * top
    bf16 = jnp.bfloat16
    dma = pltpu.SemaphoreType.DMA
    vmem = pl.BlockSpec(memory_space=pltpu.VMEM)
    hbm = pl.BlockSpec(memory_space=pl.ANY)
    parts = pl.pallas_call(
        kernel,
        out_shape=(
            pltpu.VMEM((choices, 2 * hidden), bf16),
            pltpu.VMEM((2, RING, CAP, hidden), bf16),
            pltpu.VMEM((choices, RING * CAP), bf16),
            pltpu.VMEM((choices, 128), jnp.float32),
        ),
        in_specs=[hbm, hbm, vmem, vmem],
        out_specs=[vmem] * 4,
        scratch_shapes=[
            pltpu.VMEM((RING, 2 * local_tokens, width), bf16),
            pltpu.VMEM((RING, hidden, width), bf16),
            pltpu.VMEM((RING, RING * PAIR, width), bf16),
            *[pltpu.VMEM((2 * RING, len(g) * CAP, hidden), bf16) for g in GROUPS],
            *[pltpu.VMEM((2, RING, len(g) * CAP, hidden), bf16) for g in GROUPS[:-1]],
            pltpu.VMEM((choices, STARTS[-1]), bf16),
            pltpu.VMEM((RING, 2, top, local_tokens), jnp.int32),
            pltpu.VMEM((RING, 2, RING, local_tokens), jnp.float32),
            dma((2,)),
            dma(()),
            dma((2, 7)),
            dma(()),
            dma((2, 7)),
            dma((2,)),
            dma(()),
            dma((2, 7)),
            dma(()),
            dma((2, 7)),
            dma(()),
            dma((2, 4)),
            dma(()),
            dma((2, 4)),
            dma((len(GROUPS),)),
            dma((len(GROUPS),)),
            dma((len(GROUPS),)),
            dma((len(GROUPS),)),
        ],
        compiler_params=pltpu.CompilerParams(
            collective_id=0, has_side_effects=True, vmem_limit_bytes=52 * 2**20
        ),
    )(expert_down, out_grad, routes.T, gates.T)
    steps = 8
    final = pl.pallas_call(
        finish_kernel,
        out_shape=jax.ShapeDtypeStruct((choices, 2 * hidden), bf16),
        in_specs=[vmem] * 4,
        out_specs=hbm,
        scratch_shapes=[
            pltpu.VMEM((steps, choices // steps, 2 * hidden), bf16),
            dma((steps,)),
        ],
        compiler_params=pltpu.CompilerParams(vmem_limit_bytes=16 * 2**20),
    )(*parts)
    return final.reshape(local_tokens, top, 2 * hidden)


def solution(mesh):
    placed = (
        P("expert", None),
        P(("dp", "expert"), None),
        P(("dp", "expert"), None),
        P(("dp", "expert"), None),
    )
    return jax.shard_map(
        shards,
        mesh=mesh,
        in_specs=placed,
        out_specs=P(("dp", "expert"), None, None),
        check_vma=False,
    )
```
